128 devices in a mesh: lat: 4 (over x_lo, core), lon: 32 (over x_hi, z, y).
Axes of the slice: x: 4 (x_hi: 2, x_lo: 2; x = x_hi * 2 + x_lo), y: 4, z: 4, core: 2. Of those that a mesh axis runs over, the one named last changes fastest.
Arguments:
- nodes: bfloat16 [64, 1024, 512], P('lat', 'lon'), may hold values from -6 to 6
- edges: bfloat16 [4, 32, 16, 128, 512], P('lat', 'lon'), may hold values from -6 to 6
- senders: int32 [4, 32, 16, 128], P('lat', 'lon'), may hold values from 0 to 611, as said below
- receivers: int32 [4, 32, 16, 128], P('lat', 'lon'), may hold values from 0 to 511, as said below
- counts: int32 [4, 32, 16], P('lat', 'lon'), may hold values from 0 to 128, as said below
- cotangent: float32 [64, 1024, 512], P('lat', 'lon'), may hold values from -6 to 6
- w_edge_in: bfloat16 [1536, 512], replicated, may hold values from -0.15625 to 0.15625
- w_edge_out: bfloat16 [512, 512], replicated, may hold values from -0.25 to 0.25
- w_node_in: bfloat16 [1024, 512], replicated, may hold values from -0.1875 to 0.1875
- w_node_out: bfloat16 [512, 512], replicated, may hold values from -0.25 to 0.25
- gain_edge: float32 [512], replicated, may hold values from 0.25 to 1.75
- gain_node: float32 [512], replicated, may hold values from 0.25 to 1.75
Outputs:
- node_out: bfloat16 [64, 1024, 512], P('lat', 'lon')
- edge_out: bfloat16 [4, 32, 16, 128, 512], P('lat', 'lon')
- node_grad: bfloat16 [64, 1024, 512], P('lat', 'lon')
- edge_grad: bfloat16 [4, 32, 16, 128, 512], P('lat', 'lon')
- grad_edge_in: bfloat16 [1536, 512], replicated
- grad_edge_out: bfloat16 [512, 512], replicated
- grad_node_in: bfloat16 [1024, 512], replicated
- grad_node_out: bfloat16 [512, 512], replicated
- grad_gain_edge: float32 [512], replicated
- grad_gain_node: float32 [512], replicated
The draws below stay inside these ranges and needn't reach their ends.
Inputs may be any that keep to these rules, and one draw needn't show every extreme that they name: `senders`: each sender is one of the eight cells around its receiver's cell in the extended patch, its receiver at extended cell (receiver // 32 + 1, receiver % 32 + 1). `receivers`: edges of one slot: see senders. `counts`: on each device the blocks with live slots come first, and block 0 is full; the number of blocks with live slots differs from device to device.
All inputs are finite; a program needn't handle non-finite values.
Results may differ from the reference program's by a relative error of at most 0.009.
Values may be sent and summed in bfloat16 or wider, within the bound.
A program may use at most 192 MiB of HBM per device.

```python
import jax
import jax.numpy as jnp
from jax import lax

D = 512
PLAT = 16
PLON = 32
BLK_DEV = 16
EDGE_BLK = 128
NLAT = 64
NLONC = 1024
N_LAT = 4
N_LON = 32


def edge_ends(key):
    base_key = jax.random.fold_in(key, 7)
    key_recv, key_choose = jax.random.split(base_key)
    layout = (N_LAT, N_LON, BLK_DEV, EDGE_BLK)
    receiver = jax.random.randint(key_recv, layout, 0, PLAT * PLON, dtype=jnp.int32)
    choose = jax.random.randint(key_choose, layout, 0, 8, dtype=jnp.int32)
    row_offsets = jnp.array([-1, -1, -1, 0, 0, 1, 1, 1], jnp.int32)
    col_offsets = jnp.array([-1, 0, 1, -1, 1, -1, 0, 1], jnp.int32)
    send_row = receiver // PLON + 1 + row_offsets[choose]
    send_col = receiver % PLON + 1 + col_offsets[choose]
    return (send_row * (PLON + 2) + send_col, receiver)


def draw_senders(key, part):
    return edge_ends(key)[0]


def draw_receivers(key, part):
    return edge_ends(key)[1]


def draw_counts(key, part):
    base_key = jax.random.fold_in(key, 13)
    key_active, key_fill = jax.random.split(base_key)
    active = jax.random.randint(key_active, (N_LAT, N_LON, 1), 1, BLK_DEV + 1, dtype=jnp.int32)
    filled = jax.random.randint(key_fill, (N_LAT, N_LON, BLK_DEV), EDGE_BLK // 2, EDGE_BLK + 1, dtype=jnp.int32)
    position = jnp.arange(BLK_DEV, dtype=jnp.int32)[None, None, :]
    result = jnp.where(position < active, filled, 0)
    return jnp.where(position == 0, EDGE_BLK, result).astype(jnp.int32)


def block_scale(own_key, extent, cuts, smallest, largest):
    loudness = 1.0
    for dim, blocks in cuts:
        steps = jax.random.uniform(jax.random.fold_in(jax.random.fold_in(own_key, 6), dim), (blocks,), jnp.float32, smallest / len(cuts), largest / len(cuts))
        loudness = loudness * jnp.repeat(jnp.exp(steps), extent[dim] // blocks).reshape((-1,) + (1,) * (len(extent) - 1 - dim))
    return loudness


def noise(stream_key, shape, scale, reach, cuts=(), kind=jnp.bfloat16):
    entries = scale * jax.random.normal(stream_key, shape, jnp.float32)
    if cuts:
        entries = entries * block_scale(stream_key, shape, cuts, -0.22, 0.18)
    return jnp.clip(entries, -reach, reach).astype(kind)


def setup_inputs(seed: int = 0) -> dict:
    splits = jax.random.split(jax.random.key(seed), 13)
    return {
        "nodes": noise(splits[0], (NLAT, NLONC, D), 1.0, 6.0, ((0, 4), (1, 32))),
        "edges": noise(splits[1], (N_LAT, N_LON, BLK_DEV, EDGE_BLK, D), 1.0, 6.0, ((0, 4), (1, 32))),
        "senders": draw_senders(jax.random.fold_in(splits[12], 71), 0),
        "receivers": draw_receivers(jax.random.fold_in(splits[12], 71), 0),
        "counts": draw_counts(jax.random.fold_in(splits[12], 71), 0),
        "cotangent": noise(splits[5], (NLAT, NLONC, D), 1.0, 6.0, ((0, 4), (1, 32)), jnp.float32),
        "w_edge_in": noise(splits[6], (3 * D, D), (3 * D) ** -0.5, 0.15625),
        "w_edge_out": noise(splits[7], (D, D), D ** -0.5, 0.25),
        "w_node_in": noise(splits[8], (2 * D, D), (2 * D) ** -0.5, 0.1875),
        "w_node_out": noise(splits[9], (D, D), D ** -0.5, 0.25),
        "gain_edge": jnp.clip(1.0 + 0.15 * jax.random.normal(splits[10], (D,), jnp.float32), 0.25, 1.75),
        "gain_node": jnp.clip(1.0 + 0.15 * jax.random.normal(splits[11], (D,), jnp.float32), 0.25, 1.75),
    }


EPS = 1e-05

def norm_forward(values, gain_vec):
    average = lax.optimization_barrier(jnp.mean(values, -1, keepdims=True))
    centred = values - average
    spread = lax.optimization_barrier(jnp.mean(centred * centred, -1, keepdims=True))
    inverse = lax.rsqrt(spread + EPS)
    standard = centred * inverse
    return (standard * gain_vec, standard, inverse)

def norm_backward(upstream, standard, inverse, gain_vec):
    scaled = upstream * gain_vec
    return inverse * (scaled - lax.optimization_barrier(jnp.mean(scaled, -1, keepdims=True)) - standard * lax.optimization_barrier(jnp.mean(scaled * standard, -1, keepdims=True)))

def silu_slope(values):
    logistic = jax.nn.sigmoid(values)
    return logistic * (1.0 + values * (1.0 - logistic))

def reference(nodes, edges, senders, receivers, counts, cotangent, w_edge_in, w_edge_out, w_node_in, w_node_out, gain_edge, gain_node):
    latent = nodes.shape[2]
    lat_rows = nodes.shape[0]
    lon_cols = nodes.shape[1]
    devices = N_LAT * N_LON
    padded = jnp.pad(nodes, ((1, 1), (0, 0), (0, 0)))
    padded = jnp.concatenate([padded[:, -1:], padded, padded[:, :1]], axis=1)
    table = padded.reshape(-1, latent)
    own_rows = nodes.reshape(-1, latent)
    device = jnp.arange(devices, dtype=jnp.int32)
    device_lat = (device // N_LON)[:, None]
    device_lon = (device % N_LON)[:, None]
    sending = senders.reshape(devices, -1).astype(jnp.int32)
    getting = receivers.reshape(devices, -1).astype(jnp.int32)
    send_rows = (device_lat * PLAT + sending // (PLON + 2)) * (lon_cols + 2) + device_lon * PLON + sending % (PLON + 2)
    recv_rows = (device_lat * PLAT + getting // PLON) * lon_cols + device_lon * PLON + getting % PLON
    slot_index = jnp.arange(EDGE_BLK, dtype=jnp.int32)[None, None, :]
    valid = (slot_index < counts.reshape(devices, BLK_DEV, 1).astype(jnp.int32)).astype(jnp.float32).reshape(devices, -1, 1)
    edge_rows = edges.reshape(devices, -1, latent)

    def edge_forward(block_rows, sender, receiver, live):
        stacked = jnp.concatenate([block_rows, table[sender], own_rows[receiver]], axis=1)
        preact = jnp.dot(stacked, w_edge_in, preferred_element_type=jnp.float32)
        hidden = jax.nn.silu(preact).astype(jnp.bfloat16)
        edge_mlp = jnp.dot(hidden, w_edge_out, preferred_element_type=jnp.float32)
        normed, standard, inverse = norm_forward(edge_mlp, gain_edge)
        return (stacked, preact, hidden, normed * live, standard, inverse)

    def first_pass(aggregate, inputs):
        block_rows, sender, receiver, live = inputs
        message = edge_forward(block_rows, sender, receiver, live)[3]
        updated = (block_rows.astype(jnp.float32) + message).astype(jnp.bfloat16)
        return (aggregate.at[receiver].add(message), updated)
    aggregate, edge_new = lax.scan(first_pass, jnp.zeros((own_rows.shape[0], latent), jnp.float32), (edge_rows, send_rows, recv_rows, valid))
    node_inputs = jnp.concatenate([own_rows, aggregate.astype(jnp.bfloat16)], axis=1)
    node_pre = jnp.dot(node_inputs, w_node_in, preferred_element_type=jnp.float32)
    node_hidden = jax.nn.silu(node_pre).astype(jnp.bfloat16)
    node_mlp = jnp.dot(node_hidden, w_node_out, preferred_element_type=jnp.float32)
    normed, standard, inverse = norm_forward(node_mlp, gain_node)
    node_out = (own_rows.astype(jnp.float32) + normed).astype(jnp.bfloat16)
    upstream = cotangent.reshape(-1, latent)
    grad_gain_node = lax.optimization_barrier(jnp.sum(upstream * standard, 0))
    grad_mlp = norm_backward(upstream, standard, inverse, gain_node).astype(jnp.bfloat16)
    grad_node_out = jnp.dot(node_hidden.T, grad_mlp, preferred_element_type=jnp.float32)
    grad_node_pre = (jnp.dot(grad_mlp, w_node_out.T, preferred_element_type=jnp.float32) * silu_slope(node_pre)).astype(jnp.bfloat16)
    grad_node_in = jnp.dot(node_inputs.T, grad_node_pre, preferred_element_type=jnp.float32)
    grad_inputs = jnp.dot(grad_node_pre, w_node_in.T, preferred_element_type=jnp.float32)
    direct = grad_inputs[:, :latent]
    grad_aggregate = grad_inputs[:, latent:]

    def second_pass(carry, inputs):
        sum_in, sum_out, sum_gain, grad_table, grad_own = carry
        block_rows, sender, receiver, live = inputs
        stacked, preact, hidden, message, edge_std, edge_inv = edge_forward(block_rows, sender, receiver, live)
        incoming = grad_aggregate[receiver] * live
        sum_gain = sum_gain + lax.optimization_barrier(jnp.sum(incoming * edge_std, 0))
        grad_edge_mlp = norm_backward(incoming, edge_std, edge_inv, gain_edge).astype(jnp.bfloat16)
        sum_out = sum_out + jnp.dot(hidden.T, grad_edge_mlp, preferred_element_type=jnp.float32)
        grad_hidden = jnp.dot(grad_edge_mlp, w_edge_out.T, preferred_element_type=jnp.float32)
        grad_preact = (grad_hidden * silu_slope(preact)).astype(jnp.bfloat16)
        sum_in = sum_in + jnp.dot(stacked.T, grad_preact, preferred_element_type=jnp.float32)
        grad_stack = jnp.dot(grad_preact, w_edge_in.T, preferred_element_type=jnp.float32)
        grad_table = grad_table.at[sender].add(grad_stack[:, latent:2 * latent])
        grad_own = grad_own.at[receiver].add(grad_stack[:, 2 * latent:])
        return ((sum_in, sum_out, sum_gain, grad_table, grad_own), grad_stack[:, :latent].astype(jnp.bfloat16))
    start = (jnp.zeros((3 * latent, latent), jnp.float32), jnp.zeros((latent, latent), jnp.float32), jnp.zeros((latent,), jnp.float32), jnp.zeros(table.shape, jnp.float32), jnp.zeros(own_rows.shape, jnp.float32))
    carry, edge_back = lax.scan(second_pass, start, (edge_rows, send_rows, recv_rows, valid))
    sum_in, sum_out, sum_gain, grad_table, grad_own = carry
    grad_padded = grad_table.reshape(lat_rows + 2, lon_cols + 2, latent)
    grad_padded = grad_padded.at[:, 1].add(grad_padded[:, -1])
    grad_padded = grad_padded.at[:, -2].add(grad_padded[:, 0])
    from_senders = grad_padded[1:-1, 1:-1].reshape(-1, latent)
    node_grad = (upstream + direct + grad_own + from_senders).astype(jnp.bfloat16)
    return (node_out.reshape(nodes.shape), edge_new.reshape(edges.shape), node_grad.reshape(nodes.shape), edge_back.reshape(edges.shape), sum_in.astype(jnp.bfloat16), sum_out.astype(jnp.bfloat16), grad_node_in.astype(jnp.bfloat16), grad_node_out.astype(jnp.bfloat16), sum_gain, grad_gain_node)
```

```python
import functools

import jax
import jax.numpy as jnp
from jax import lax
from jax.experimental import pallas as pl
from jax.experimental.pallas import tpu as pltpu
from jax.sharding import PartitionSpec as P

EPS = 1e-05
D = 512
ROWS = 16
COLS = 32
OWN = ROWS * COLS
RIM = 160
RIM_PAD = 256
CELLS = OWN + RIM
BLOCKS = 16
SLOTS = 128
EDGES = BLOCKS * SLOTS
CHUNK = 512
STEPS = EDGES // CHUNK
PER = CHUNK // SLOTS
TABLE = OWN + RIM_PAD + OWN
F32 = jnp.float32
BF16 = jnp.bfloat16
VMEM_LIMIT = 63 * 1024 * 1024

ROUTES = (
    (-1, 0, 0, 32, 32),
    (1, 0, 32, 32, 0),
    (0, -1, 64, 16, 80),
    (0, 1, 80, 16, 64),
    (-1, -1, 96, 16, 144),
    (-1, 1, 112, 16, 128),
    (1, -1, 128, 16, 112),
    (1, 1, 144, 16, 96),
)


def dot(a, b):
    return lax.dot_general(a, b, (((1,), (0,)), ((), ())), preferred_element_type=F32)


def dot_bt(a, b):
    return lax.dot_general(a, b, (((1,), (1,)), ((), ())), preferred_element_type=F32)


def dot_at(a, b):
    return lax.dot_general(a, b, (((0,), (0,)), ((), ())), preferred_element_type=F32)


def rim_nodes(r):
    t = jnp.where(r < 32, r, 448 + r)
    t = jnp.where(r >= 64, (r - 64) * 32, t)
    t = jnp.where(r >= 80, (r - 80) * 32 + 31, t)
    t = jnp.where(r >= 96, -1, t)
    t = jnp.where(r == 96, 0, t)
    t = jnp.where(r == 112, 31, t)
    t = jnp.where(r == 128, 480, t)
    return jnp.where(r == 144, 511, t)


def rim_picks(rim_axis):
    shape = (RIM, OWN) if rim_axis == 0 else (OWN, RIM)
    r = lax.broadcasted_iota(jnp.int32, shape, rim_axis)
    n = lax.broadcasted_iota(jnp.int32, shape, 1 - rim_axis)
    return (rim_nodes(r) == n).astype(F32).astype(BF16)


def exchange(send_buf, recv_buf, send_sem, recv_sem, prepare):
    lat = lax.axis_index("lat")
    lon = lax.axis_index("lon")
    count = lax.axis_size("lon")
    bands = lax.axis_size("lat")
    recv_buf[...] = jnp.zeros_like(recv_buf)
    prepare()
    barrier = pltpu.get_barrier_semaphore()

    def present(step):
        return jnp.logical_and(lat + step >= 0, lat + step < bands)

    def target(step, turn):
        return {"lat": lat + step, "lon": lax.rem(lon + turn + count, count)}

    for step, turn, _, _, _ in ROUTES:

        @pl.when(present(step))
        def _():
            pl.semaphore_signal(
                barrier, inc=1, device_id=target(step, turn), device_id_type=pl.DeviceIdType.MESH
            )

    up = (lat > 0).astype(jnp.int32)
    down = (lat < bands - 1).astype(jnp.int32)
    pl.semaphore_wait(barrier, 2 + 3 * up + 3 * down)

    def copy(k):
        step, turn, start, rows, land = ROUTES[k]
        return pltpu.make_async_remote_copy(
            src_ref=send_buf.at[pl.ds(start, rows)],
            dst_ref=recv_buf.at[pl.ds(land, rows)],
            send_sem=send_sem.at[k],
            recv_sem=recv_sem.at[k],
            device_id=target(step, turn),
            device_id_type=pl.DeviceIdType.MESH,
        )

    for k, route in enumerate(ROUTES):

        @pl.when(present(route[0]))
        def _():
            copy(k).start()

    for k, route in enumerate(ROUTES):

        @pl.when(present(route[0]))
        def _():
            copy(k).wait_send()

        @pl.when(present(-route[0]))
        def _():
            copy(k).wait_recv()


def halo_kernel(nodes, rim, send_buf, recv_buf, send_sem, recv_sem):
    def prepare():
        send_buf[...] = dot(rim_picks(0), nodes[...]).astype(BF16)

    exchange(send_buf, recv_buf, send_sem, recv_sem, prepare)
    rim[...] = recv_buf[...]


def return_kernel(rim_grad, base, node_grad, send_buf, recv_buf, send_sem, recv_sem):
    def prepare():
        send_buf[...] = rim_grad[...]

    exchange(send_buf, recv_buf, send_sem, recv_sem, prepare)
    node_grad[...] = (base[...] + dot(rim_picks(1), recv_buf[...])).astype(BF16)


RIM_SCRATCH = [
    pltpu.VMEM((RIM, D), BF16),
    pltpu.VMEM((RIM, D), BF16),
    pltpu.SemaphoreType.DMA((len(ROUTES),)),
    pltpu.SemaphoreType.DMA((len(ROUTES),)),
]


def whole(n):
    return [pl.BlockSpec(memory_space=pltpu.VMEM)] * n


def halo(nodes):
    return pl.pallas_call(
        halo_kernel,
        out_shape=jax.ShapeDtypeStruct((RIM, D), BF16),
        in_specs=whole(1),
        out_specs=whole(1)[0],
        scratch_shapes=RIM_SCRATCH,
        compiler_params=pltpu.CompilerParams(collective_id=0, has_side_effects=True),
        name="halo",
    )(nodes)


def give_back(rim_grad, base):
    return pl.pallas_call(
        return_kernel,
        out_shape=jax.ShapeDtypeStruct((OWN, D), BF16),
        in_specs=whole(2),
        out_specs=whole(1)[0],
        scratch_shapes=RIM_SCRATCH,
        compiler_params=pltpu.CompilerParams(collective_id=1, has_side_effects=True),
        name="give_back",
    )(rim_grad, base)


def normalize(values):
    average = jnp.mean(values, -1, keepdims=True)
    centred = values - average
    spread = jnp.mean(centred * centred, -1, keepdims=True)
    inverse = lax.rsqrt(spread + EPS)
    return centred * inverse, inverse


def norm_backward(scaled, standard, inverse):
    return inverse * (
        scaled
        - jnp.mean(scaled, -1, keepdims=True)
        - standard * jnp.mean(scaled * standard, -1, keepdims=True)
    )


def silu_parts(values):
    logistic = 1.0 / (1.0 + jnp.exp(-values))
    hidden = values * logistic
    return hidden, logistic * (1.0 + values * (1.0 - logistic))


def cell_rows(senders):
    row = (senders * 1928) >> 16
    col = senders - row * 34
    left, right = col == 0, col == 33
    top, bottom = row == 0, row == 17
    place = (row - 1) * 32 + col - 1
    place = jnp.where(top, OWN + col - 1, place)
    place = jnp.where(bottom, OWN + 32 + col - 1, place)
    place = jnp.where(left, OWN + 64 + row - 1, place)
    place = jnp.where(right, OWN + 80 + row - 1, place)
    place = jnp.where(jnp.logical_and(top, left), OWN + 96, place)
    place = jnp.where(jnp.logical_and(top, right), OWN + 112, place)
    place = jnp.where(jnp.logical_and(bottom, left), OWN + 128, place)
    return jnp.where(jnp.logical_and(bottom, right), OWN + 144, place)


def one_hot(mask):
    return jnp.where(mask, 1.0, 0.0).astype(BF16)


def picks_by_slot(ids, width):
    parts = []
    for k in range(PER):
        column = jnp.broadcast_to(ids[k : k + 1], (SLOTS, SLOTS)).T
        lanes = lax.broadcasted_iota(jnp.int32, (SLOTS, SLOTS), 1)
        parts.append(
            jnp.concatenate([one_hot(column == lanes + s) for s in range(0, width, SLOTS)], axis=1)
        )
    return jnp.concatenate(parts, axis=0)


def picks_by_row(ids, height):
    rows = lax.broadcasted_iota(jnp.int32, (height, SLOTS), 0)
    return jnp.concatenate([one_hot(rows == ids[k : k + 1]) for k in range(PER)], axis=1)


def local_kernel(
    counts,
    nodes,
    rim,
    edges,
    senders,
    receivers,
    cotangent,
    w_edge_in,
    w_edge_out,
    w_node_in,
    w_node_out,
    gain_edge,
    gain_node,
    node_out,
    edge_out,
    edge_grad,
    base,
    rim_grad,
    g_edge_in,
    g_edge_out,
    g_node_in,
    g_node_out,
    g_gain,
    proj,
    cells,
    hidden_all,
    slope_all,
    std_all,
    inv_all,
    agg,
    acc_send,
    acc_recv,
    acc_in,
    acc_out,
    grad_agg,
):
    own = nodes[...]
    cells[...] = cell_rows(senders[...])
    w_mid = w_edge_in[pl.ds(D, D)]
    proj[pl.ds(0, OWN)] = dot(own, w_mid).astype(BF16)
    proj[pl.ds(OWN, RIM)] = dot(rim[...], w_mid).astype(BF16)
    proj[pl.ds(CELLS, RIM_PAD - RIM)] = jnp.zeros((RIM_PAD - RIM, D), BF16)
    proj[pl.ds(OWN + RIM_PAD, OWN)] = dot(own, w_edge_in[pl.ds(2 * D, D)]).astype(BF16)

    agg[...] = jnp.zeros_like(agg)
    acc_send[...] = jnp.zeros_like(acc_send)
    acc_recv[...] = jnp.zeros_like(acc_recv)
    acc_in[...] = jnp.zeros_like(acc_in)
    acc_out[...] = jnp.zeros_like(acc_out)

    def live(step):
        slot = lax.broadcasted_iota(jnp.int32, (SLOTS, 1), 0)
        return jnp.concatenate(
            [jnp.where(slot < counts[step * PER + k], 1.0, 0.0) for k in range(PER)], axis=0
        )

    def forward(step, carry):
        span = pl.ds(pl.multiple_of(step * CHUNK, CHUNK), CHUNK)
        blocks = pl.ds(step * PER, PER)
        block = edges[span]
        recv_ids = receivers[blocks]
        picks = jnp.concatenate(
            [picks_by_slot(cells[blocks], OWN + RIM_PAD), picks_by_slot(recv_ids, OWN)], axis=1
        )
        pre = dot(block, w_edge_in[pl.ds(0, D)]) + dot(picks, proj[...])
        hidden, slope = silu_parts(pre)
        hidden = hidden.astype(BF16)
        hidden_all[span] = hidden
        slope_all[span] = slope
        standard, inverse = normalize(dot(hidden, w_edge_out[...]))
        std_all[span] = standard
        inv_all[span] = inverse
        message = standard * gain_edge[...] * live(step)
        edge_out[span] = (block.astype(F32) + message).astype(BF16)
        agg[...] += dot(picks_by_row(recv_ids, OWN), message.astype(BF16))
        return carry

    lax.fori_loop(0, STEPS, forward, 0)

    sums = agg[...].astype(BF16)
    node_pre = dot(own, w_node_in[pl.ds(0, D)]) + dot(sums, w_node_in[pl.ds(D, D)])
    node_hidden, node_slope = silu_parts(node_pre)
    node_hidden = node_hidden.astype(BF16)
    node_std, node_inv = normalize(dot(node_hidden, w_node_out[...]))
    node_out[...] = (own.astype(F32) + node_std * gain_node[...]).astype(BF16)
    upstream = cotangent[...]
    gain_sum_node = jnp.sum(upstream * node_std, 0, keepdims=True)
    grad_mlp = norm_backward(upstream * gain_node[...], node_std, node_inv).astype(BF16)
    g_node_out[...] = dot_at(node_hidden, grad_mlp).astype(BF16)
    grad_node_pre = (dot_bt(grad_mlp, w_node_out[...]) * node_slope).astype(BF16)
    g_node_in[pl.ds(0, D)] = dot_at(own, grad_node_pre).astype(BF16)
    g_node_in[pl.ds(D, D)] = dot_at(sums, grad_node_pre).astype(BF16)
    base[...] = upstream + dot_bt(grad_node_pre, w_node_in[pl.ds(0, D)])
    grad_agg[...] = dot_bt(grad_node_pre, w_node_in[pl.ds(D, D)]).astype(BF16)

    def backward(step, gain_sum):
        span = pl.ds(pl.multiple_of(step * CHUNK, CHUNK), CHUNK)
        blocks = pl.ds(step * PER, PER)
        recv_ids = receivers[blocks]
        standard = std_all[span]
        incoming = dot(picks_by_slot(recv_ids, OWN), grad_agg[...]) * live(step)
        gain_sum = gain_sum + jnp.sum(incoming * standard, 0, keepdims=True)
        grad_norm = norm_backward(incoming * gain_edge[...], standard, inv_all[span]).astype(BF16)
        acc_out[...] += dot_at(hidden_all[span], grad_norm)
        grad_pre = (dot_bt(grad_norm, w_edge_out[...]) * slope_all[span]).astype(BF16)
        acc_in[...] += dot_at(edges[span], grad_pre)
        edge_grad[span] = dot_bt(grad_pre, w_edge_in[pl.ds(0, D)]).astype(BF16)
        acc_send[...] += dot(picks_by_row(cells[blocks], CELLS), grad_pre)
        acc_recv[...] += dot(picks_by_row(recv_ids, OWN), grad_pre)
        return gain_sum

    gain_sum_edge = lax.fori_loop(0, STEPS, backward, jnp.zeros((1, D), F32))
    g_gain[...] = jnp.concatenate(
        [gain_sum_edge, gain_sum_node, jnp.zeros((6, D), F32)], axis=0
    )
    g_edge_out[...] = acc_out[...].astype(BF16)
    g_edge_in[pl.ds(0, D)] = acc_in[...].astype(BF16)
    by_send = acc_send[...].astype(BF16)
    by_recv = acc_recv[...].astype(BF16)
    g_edge_in[pl.ds(D, D)] = (dot_at(own, by_send[:OWN]) + dot_at(rim[...], by_send[OWN:])).astype(
        BF16
    )
    g_edge_in[pl.ds(2 * D, D)] = dot_at(own, by_recv).astype(BF16)
    rim_grad[...] = dot_bt(by_send[OWN:], w_mid).astype(BF16)
    base[...] += dot_bt(by_send[:OWN], w_mid) + dot_bt(by_recv, w_edge_in[pl.ds(2 * D, D)])


def local(counts, *rest):
    shapes = [
        ((OWN, D), BF16),
        ((EDGES, D), BF16),
        ((EDGES, D), BF16),
        ((OWN, D), F32),
        ((RIM, D), BF16),
        ((3 * D, D), BF16),
        ((D, D), BF16),
        ((2 * D, D), BF16),
        ((D, D), BF16),
        ((8, D), F32),
    ]
    scratch = [
        ((TABLE, D), BF16),
        ((BLOCKS, SLOTS), jnp.int32),
        ((EDGES, D), BF16),
        ((EDGES, D), F32),
        ((EDGES, D), F32),
        ((EDGES, 1), F32),
        ((OWN, D), F32),
        ((CELLS, D), F32),
        ((OWN, D), F32),
        ((D, D), F32),
        ((D, D), F32),
        ((OWN, D), BF16),
    ]
    return pl.pallas_call(
        local_kernel,
        out_shape=[jax.ShapeDtypeStruct(s, t) for s, t in shapes],
        in_specs=[pl.BlockSpec(memory_space=pltpu.SMEM)] + whole(len(rest)),
        out_specs=whole(len(shapes)),
        scratch_shapes=[pltpu.VMEM(s, t) for s, t in scratch],
        compiler_params=pltpu.CompilerParams(vmem_limit_bytes=VMEM_LIMIT),
        name="local",
    )(counts, *rest)


def shards(
    nodes,
    edges,
    senders,
    receivers,
    counts,
    cotangent,
    w_edge_in,
    w_edge_out,
    w_node_in,
    w_node_out,
    gain_edge,
    gain_node,
):
    own = nodes.reshape(OWN, D)
    rim = halo(own)
    (
        node_out,
        edge_out,
        edge_grad,
        base,
        rim_grad,
        g_edge_in,
        g_edge_out,
        g_node_in,
        g_node_out,
        g_gain,
    ) = local(
        counts.reshape(BLOCKS),
        own,
        rim,
        edges.reshape(EDGES, D),
        senders.reshape(BLOCKS, SLOTS),
        receivers.reshape(BLOCKS, SLOTS),
        cotangent.reshape(OWN, D),
        w_edge_in,
        w_edge_out,
        w_node_in,
        w_node_out,
        gain_edge.reshape(1, D),
        gain_node.reshape(1, D),
    )
    node_grad = give_back(rim_grad, base)
    summed = lax.psum((g_edge_in, g_edge_out, g_node_in, g_node_out), ("lat", "lon"))
    gains = lax.psum(g_gain, ("lat", "lon"))
    return (
        node_out.reshape(nodes.shape),
        edge_out.reshape(edges.shape),
        node_grad.reshape(nodes.shape),
        edge_grad.reshape(edges.shape),
        *summed,
        gains[0],
        gains[1],
    )


def solution(mesh):
    in_specs = (
        P("lat", "lon", None),
        P("lat", "lon", None, None, None),
        P("lat", "lon", None, None),
        P("lat", "lon", None, None),
        P("lat", "lon", None),
        P("lat", "lon", None),
        P(),
        P(),
        P(),
        P(),
        P(),
        P(),
    )
    out_specs = (
        P("lat", "lon", None),
        P("lat", "lon", None, None, None),
        P("lat", "lon", None),
        P("lat", "lon", None, None, None),
        P(),
        P(),
        P(),
        P(),
        P(),
        P(),
    )
    return jax.shard_map(shards, mesh=mesh, in_specs=in_specs, out_specs=out_specs, check_vma=False)
```

```python
import functools

import jax
import jax.numpy as jnp
from jax import lax
from jax.experimental import pallas as pl
from jax.experimental.pallas import tpu as pltpu
from jax.sharding import PartitionSpec as P

EPS = 1e-05
D = 512
ROWS = 16
COLS = 32
OWN = ROWS * COLS
RIM = 160
RIM_PAD = 256
CELLS = OWN + RIM
BLOCKS = 16
SLOTS = 128
EDGES = BLOCKS * SLOTS
CHUNK = 512
STEPS = EDGES // CHUNK
PER = CHUNK // SLOTS
TABLE = OWN + RIM_PAD + OWN
F32 = jnp.float32
BF16 = jnp.bfloat16
VMEM_LIMIT = 63 * 1024 * 1024

LANES = 128
AT_EDGE_IN = 0
AT_EDGE_OUT = AT_EDGE_IN + 4 * 3 * D
AT_NODE_IN = AT_EDGE_OUT + 4 * D
AT_NODE_OUT = AT_NODE_IN + 4 * 2 * D
AT_GAINS = AT_NODE_OUT + 4 * D
PACKED = 15360
HALF = PACKED // 2
PARTS = 3
PART = HALF // PARTS
PHASES = 3
TURN = ((0, 1, 2), (1, 2, 0), (2, 0, 1))
PIECE = (PART // 4, PART // 16, PART // 64)
FIRST = (PIECE[0] // 2, PIECE[1] // 2, 24)
HOPS = 6
MESH = pl.DeviceIdType.MESH

ROUTES = (
    (-1, 0, 0, 32, 32),
    (1, 0, 32, 32, 0),
    (0, -1, 64, 16, 80),
    (0, 1, 80, 16, 64),
    (-1, -1, 96, 16, 144),
    (-1, 1, 112, 16, 128),
    (1, -1, 128, 16, 112),
    (1, 1, 144, 16, 96),
)


def dot(a, b):
    return lax.dot_general(a, b, (((1,), (0,)), ((), ())), preferred_element_type=F32)


def dot_bt(a, b):
    return lax.dot_general(a, b, (((1,), (1,)), ((), ())), preferred_element_type=F32)


def dot_at(a, b):
    return lax.dot_general(a, b, (((0,), (0,)), ((), ())), preferred_element_type=F32)


def rim_nodes(r):
    t = jnp.where(r < 32, r, 448 + r)
    t = jnp.where(r >= 64, (r - 64) * 32, t)
    t = jnp.where(r >= 80, (r - 80) * 32 + 31, t)
    t = jnp.where(r >= 96, -1, t)
    t = jnp.where(r == 96, 0, t)
    t = jnp.where(r == 112, 31, t)
    t = jnp.where(r == 128, 480, t)
    return jnp.where(r == 144, 511, t)


def rim_picks(rim_axis):
    shape = (RIM, OWN) if rim_axis == 0 else (OWN, RIM)
    r = lax.broadcasted_iota(jnp.int32, shape, rim_axis)
    n = lax.broadcasted_iota(jnp.int32, shape, 1 - rim_axis)
    return (rim_nodes(r) == n).astype(F32).astype(BF16)


class Rim:
    def __init__(self, send_buf, recv_buf, send_sem, recv_sem):
        self.refs = (send_buf, recv_buf, send_sem, recv_sem)
        self.lat, self.lon = lax.axis_index("lat"), lax.axis_index("lon")
        self.count, self.bands = lax.axis_size("lon"), lax.axis_size("lat")

    def present(self, step):
        return jnp.logical_and(self.lat + step >= 0, self.lat + step < self.bands)

    def target(self, step, turn):
        lon = lax.rem(self.lon + turn + self.count, self.count)
        return {"lat": self.lat + step, "lon": lon}

    def greet(self, barrier):
        for step, turn, _, _, _ in ROUTES:

            @pl.when(self.present(step))
            def _():
                pl.semaphore_signal(
                    barrier, inc=1, device_id=self.target(step, turn), device_id_type=MESH
                )

        up = (self.lat > 0).astype(jnp.int32)
        down = (self.lat < self.bands - 1).astype(jnp.int32)
        return 2 + 3 * up + 3 * down

    def copy(self, k):
        send_buf, recv_buf, send_sem, recv_sem = self.refs
        step, turn, start, rows, land = ROUTES[k]
        return pltpu.make_async_remote_copy(
            src_ref=send_buf.at[pl.ds(start, rows)],
            dst_ref=recv_buf.at[pl.ds(land, rows)],
            send_sem=send_sem.at[k],
            recv_sem=recv_sem.at[k],
            device_id=self.target(step, turn),
            device_id_type=MESH,
        )

    def start(self):
        for k, route in enumerate(ROUTES):

            @pl.when(self.present(route[0]))
            def _():
                self.copy(k).start()

    def wait(self):
        for k, route in enumerate(ROUTES):

            @pl.when(self.present(route[0]))
            def _():
                self.copy(k).wait_send()

            @pl.when(self.present(-route[0]))
            def _():
                self.copy(k).wait_recv()


def halo_kernel(nodes, out, send_buf, recv_buf, send_sem, recv_sem):
    rim = Rim(send_buf, recv_buf, send_sem, recv_sem)
    recv_buf[...] = jnp.zeros_like(recv_buf)
    send_buf[...] = dot(rim_picks(0), nodes[...]).astype(BF16)
    barrier = pltpu.get_barrier_semaphore()
    pl.semaphore_wait(barrier, rim.greet(barrier))
    rim.start()
    rim.wait()
    out[...] = recv_buf[...]


class Torus:
    def __init__(self):
        self.lat, self.lon = lax.axis_index("lat"), lax.axis_index("lon")
        self.core = lax.rem(self.lat, 2)
        x = (self.lon // 16) * 2 + self.lat // 2
        self.at = (x, lax.rem(self.lon, 4), lax.rem(self.lon // 4, 4))

    def near(self, axis, step):
        there = lax.rem(self.at[axis] + step + 4, 4)
        if axis == 0:
            lat = lax.rem(there, 2) * 2 + self.core
            return {"lat": lat, "lon": (there // 2) * 16 + lax.rem(self.lon, 16)}
        stride = 1 if axis == 1 else 4
        return {"lat": self.lat, "lon": self.lon + stride * (there - self.at[axis])}

    def partner(self):
        return {"lat": self.lat + 1 - 2 * self.core, "lon": self.lon}


def rows(start, size):
    return pl.ds(pl.multiple_of(start, 8), size)


def combine_kernel(
    packed,
    rim_grad,
    total,
    rim_out,
    rim_buf,
    from_core,
    wide0,
    wide1,
    wide2,
    thin0,
    thin1,
    thin2,
    first0,
    first1,
    first2,
    last0,
    last1,
    last2,
    rim_send,
    rim_recv,
    core_send,
    core_recv,
    sum_send,
    sum_recv,
    share_send,
    share_recv,
    give_send,
    give_recv,
):
    torus = Torus()
    rim = Rim(rim_grad, rim_buf, rim_send, rim_recv)
    wide, thin = (wide0, wide1, wide2), (thin0, thin1, thin2)
    first, last = (first0, first1, first2), (last0, last1, last2)
    mine = torus.core * HALF
    other = HALF - mine
    sent = []

    def send(src, dst, send_sem, recv_sem, device):
        copy = pltpu.make_async_remote_copy(
            src_ref=src,
            dst_ref=dst,
            send_sem=send_sem,
            recv_sem=recv_sem,
            device_id=device,
            device_id_type=MESH,
        )
        copy.start()
        sent.append(copy)
        return copy

    rim_buf[...] = jnp.zeros_like(rim_buf)
    barrier = pltpu.get_barrier_semaphore()
    for device in [torus.near(axis, step) for axis in range(3) for step in (1, -1)] + [
        torus.partner()
    ]:
        pl.semaphore_signal(barrier, inc=1, device_id=device, device_id_type=MESH)
    pl.semaphore_wait(barrier, 7 + rim.greet(barrier))

    from_partner = [
        send(
            packed.at[rows(other + p * PART, PART)],
            from_core.at[pl.ds(p * PART, PART)],
            core_send.at[p],
            core_recv.at[p],
            torus.partner(),
        )
        for p in range(PARTS)
    ]

    def place(p, f):
        return torus.at[TURN[p][f]]

    def piece_row(p, f, shift):
        return lax.rem(place(p, f) + shift + 4, 4) * PIECE[f]

    coming = {}

    def open_sum(p, f):
        axis, half = TURN[p][f], FIRST[f]
        rest = PIECE[f] - half
        right, left = torus.near(axis, 1), torus.near(axis, -1)
        base = (p * PHASES + f) * HOPS
        start = p * 4 * PIECE[f]

        def go(k, row, size, buf, slot, device):
            coming[p, f, k] = send(
                thin[f].at[rows(start + row, size)],
                buf.at[p * 3 + slot],
                sum_send.at[base + k],
                sum_recv.at[base + k],
                device,
            )

        go(0, piece_row(p, f, 2), half, first[f], 0, right)
        go(1, piece_row(p, f, 2) + half, rest, last[f], 0, left)
        go(2, piece_row(p, f, 1) + half, rest, last[f], 1, right)
        go(3, piece_row(p, f, -1), half, first[f], 1, left)

    def join_sum(p, f):
        axis, half = TURN[p][f], FIRST[f]
        rest = PIECE[f] - half
        base = (p * PHASES + f) * HOPS
        start = p * 4 * PIECE[f]

        def go(k, row, size, buf, device):
            coming[p, f, k - 4].wait_recv()
            joined = buf[p * 3].astype(F32) + wide[f][rows(start + row, size)]
            buf[9 + p] = joined.astype(BF16)
            coming[p, f, k] = send(
                buf.at[9 + p],
                buf.at[p * 3 + 2],
                sum_send.at[base + k],
                sum_recv.at[base + k],
                device,
            )

        go(4, piece_row(p, f, 1), half, first[f], torus.near(axis, 1))
        go(5, piece_row(p, f, -1) + half, rest, last[f], torus.near(axis, -1))

    def close_sum(p, f):
        half = FIRST[f]
        rest = PIECE[f] - half
        start = p * 4 * PIECE[f] + piece_row(p, f, 0)
        for k in (3, 2, 4, 5):
            coming[p, f, k].wait_recv()
        for offset, size, buf in ((0, half, first[f]), (half, rest, last[f])):
            value = (
                wide[f][rows(start + offset, size)]
                + buf[p * 3 + 1].astype(F32)
                + buf[p * 3 + 2].astype(F32)
            )
            if f + 1 < PHASES:
                onto = pl.ds(p * PIECE[f] + offset, size)
                wide[f + 1][onto] = value
                thin[f + 1][onto] = value.astype(BF16)
            else:
                total[rows(block_row(p, f, 0) + offset, size)] = value.astype(BF16)

    def block_row(p, f, shift):
        row = mine + p * PART + piece_row(p, f, shift)
        for g in range(f):
            row = row + piece_row(p, g, 0)
        return row

    for p in range(PARTS):
        from_partner[p].wait_recv()
        own = pl.ds(p * PART, PART)
        value = packed[rows(mine + p * PART, PART)].astype(F32) + from_core[own].astype(F32)
        wide[0][own] = value
        thin[0][own] = value.astype(BF16)
        open_sum(p, 0)
    for f in range(PHASES):
        for p in range(PARTS):
            join_sum(p, f)
        if f == 0:
            rim.start()
        for p in range(PARTS):
            close_sum(p, f)
            if f + 1 < PHASES:
                open_sum(p, f + 1)

    def share(p, f, k, shift, offset, size, device):
        region = total.at[rows(block_row(p, f, shift) + offset, size)]
        base = (p * PHASES + f) * HOPS
        coming[p, f, k] = send(
            region, region, share_send.at[base + k], share_recv.at[base + k], device
        )

    def open_share(p, f):
        axis, half = TURN[p][f], FIRST[f]
        rest = PIECE[f] - half
        right, left = torus.near(axis, 1), torus.near(axis, -1)
        share(p, f, 0, 0, 0, half, right)
        share(p, f, 1, 0, half, rest, left)
        share(p, f, 2, 0, half, rest, right)
        share(p, f, 3, 0, 0, half, left)

    def relay_share(p, f):
        axis, half = TURN[p][f], FIRST[f]
        rest = PIECE[f] - half
        coming[p, f, 0].wait_recv()
        share(p, f, 4, -1, 0, half, torus.near(axis, 1))
        coming[p, f, 1].wait_recv()
        share(p, f, 5, 1, half, rest, torus.near(axis, -1))

    given = []

    def give(p, shift, k):
        region = total.at[rows(block_row(p, 0, shift), PIECE[0])]
        given.append(
            send(
                region,
                region,
                give_send.at[p * 4 + k],
                give_recv.at[p * 4 + k],
                torus.partner(),
            )
        )

    for p in range(PARTS):
        open_share(p, PHASES - 1)
    for f in range(PHASES - 1, -1, -1):
        for p in range(PARTS):
            relay_share(p, f)
            if f == 0:
                give(p, 0, 0)
        for p in range(PARTS):
            coming[p, f, 2].wait_recv()
            if f == 0:
                give(p, -1, 1)
            coming[p, f, 3].wait_recv()
            if f == 0:
                give(p, 1, 2)
            coming[p, f, 4].wait_recv()
            coming[p, f, 5].wait_recv()
            if f == 0:
                give(p, 2, 3)
            else:
                open_share(p, f - 1)
    rim.wait()
    rim_out[...] = rim_buf[...]
    for copy in given:
        copy.wait_recv()
    for copy in sent:
        copy.wait_send()


def whole(n):
    return [pl.BlockSpec(memory_space=pltpu.VMEM)] * n


def combine(packed, rim_grad):
    dma = pltpu.SemaphoreType.DMA
    hops = PARTS * PHASES * HOPS
    scratch = [pltpu.VMEM((RIM, D), BF16), pltpu.VMEM((HALF, LANES), BF16)]
    scratch += [pltpu.VMEM((PARTS * 4 * n, LANES), F32) for n in PIECE]
    scratch += [pltpu.VMEM((PARTS * 4 * n, LANES), BF16) for n in PIECE]
    scratch += [pltpu.VMEM((12, n, LANES), BF16) for n in FIRST]
    scratch += [pltpu.VMEM((12, m - n, LANES), BF16) for m, n in zip(PIECE, FIRST)]
    scratch += [dma((n,)) for n in (8, 8, PARTS, PARTS, hops, hops, hops, hops)]
    scratch += [dma((PARTS * 4,)), dma((PARTS * 4,))]
    return pl.pallas_call(
        combine_kernel,
        out_shape=[
            jax.ShapeDtypeStruct((PACKED, LANES), BF16),
            jax.ShapeDtypeStruct((RIM, D), BF16),
        ],
        in_specs=whole(2),
        out_specs=whole(2),
        scratch_shapes=scratch,
        compiler_params=pltpu.CompilerParams(
            collective_id=1, has_side_effects=True, vmem_limit_bytes=40 * 1024 * 1024
        ),
        name="combine",
    )(packed, rim_grad)


def finish_kernel(
    total, rim_in, base, node_grad, g_edge_in, g_edge_out, g_node_in, g_node_out, gains
):
    node_grad[...] = (base[...] + dot(rim_picks(1), rim_in[...])).astype(BF16)
    for out, at in (
        (g_edge_in, AT_EDGE_IN),
        (g_edge_out, AT_EDGE_OUT),
        (g_node_in, AT_NODE_IN),
        (g_node_out, AT_NODE_OUT),
    ):
        size = out.shape[0]
        for j in range(4):
            out[:, pl.ds(j * LANES, LANES)] = total[pl.ds(at + j * size, size)]
    tail = total[pl.ds(AT_GAINS, 16)].astype(F32)
    for j in range(4):
        for k in range(2):
            gains[pl.ds(k, 1), pl.ds(j * LANES, LANES)] = tail[4 * k + j : 4 * k + j + 1]


def finish(total, rim_in, base):
    shapes = [
        ((OWN, D), BF16),
        ((3 * D, D), BF16),
        ((D, D), BF16),
        ((2 * D, D), BF16),
        ((D, D), BF16),
        ((2, D), F32),
    ]
    return pl.pallas_call(
        finish_kernel,
        out_shape=[jax.ShapeDtypeStruct(s, t) for s, t in shapes],
        in_specs=whole(3),
        out_specs=whole(len(shapes)),
        name="finish",
    )(total, rim_in, base)


RIM_SCRATCH = [
    pltpu.VMEM((RIM, D), BF16),
    pltpu.VMEM((RIM, D), BF16),
    pltpu.SemaphoreType.DMA((len(ROUTES),)),
    pltpu.SemaphoreType.DMA((len(ROUTES),)),
]


def halo(nodes):
    return pl.pallas_call(
        halo_kernel,
        out_shape=jax.ShapeDtypeStruct((RIM, D), BF16),
        in_specs=whole(1),
        out_specs=whole(1)[0],
        scratch_shapes=RIM_SCRATCH,
        compiler_params=pltpu.CompilerParams(collective_id=0, has_side_effects=True),
        name="halo",
    )(nodes)


def normalize(values):
    average = jnp.mean(values, -1, keepdims=True)
    centred = values - average
    spread = jnp.mean(centred * centred, -1, keepdims=True)
    inverse = lax.rsqrt(spread + EPS)
    return centred * inverse, inverse


def norm_backward(scaled, standard, inverse):
    return inverse * (
        scaled
        - jnp.mean(scaled, -1, keepdims=True)
        - standard * jnp.mean(scaled * standard, -1, keepdims=True)
    )


def silu_parts(values):
    logistic = 1.0 / (1.0 + jnp.exp(-values))
    hidden = values * logistic
    return hidden, logistic * (1.0 + values * (1.0 - logistic))


def cell_rows(senders):
    row = (senders * 1928) >> 16
    col = senders - row * 34
    left, right = col == 0, col == 33
    top, bottom = row == 0, row == 17
    place = (row - 1) * 32 + col - 1
    place = jnp.where(top, OWN + col - 1, place)
    place = jnp.where(bottom, OWN + 32 + col - 1, place)
    place = jnp.where(left, OWN + 64 + row - 1, place)
    place = jnp.where(right, OWN + 80 + row - 1, place)
    place = jnp.where(jnp.logical_and(top, left), OWN + 96, place)
    place = jnp.where(jnp.logical_and(top, right), OWN + 112, place)
    place = jnp.where(jnp.logical_and(bottom, left), OWN + 128, place)
    return jnp.where(jnp.logical_and(bottom, right), OWN + 144, place)


def one_hot(mask):
    return jnp.where(mask, 1.0, 0.0).astype(BF16)


def picks_by_slot(ids, width):
    parts = []
    for k in range(PER):
        column = jnp.broadcast_to(ids[k : k + 1], (SLOTS, SLOTS)).T
        lanes = lax.broadcasted_iota(jnp.int32, (SLOTS, SLOTS), 1)
        parts.append(
            jnp.concatenate([one_hot(column == lanes + s) for s in range(0, width, SLOTS)], axis=1)
        )
    return jnp.concatenate(parts, axis=0)


def picks_by_row(ids, height):
    rows = lax.broadcasted_iota(jnp.int32, (height, SLOTS), 0)
    return jnp.concatenate([one_hot(rows == ids[k : k + 1]) for k in range(PER)], axis=1)


def local_kernel(
    counts,
    nodes,
    rim,
    edges,
    senders,
    receivers,
    cotangent,
    w_edge_in,
    w_edge_out,
    w_node_in,
    w_node_out,
    gain_edge,
    gain_node,
    node_out,
    edge_out,
    edge_grad,
    base,
    rim_grad,
    packed,
    proj,
    cells,
    hidden_all,
    slope_all,
    std_all,
    inv_all,
    agg,
    acc_send,
    acc_recv,
    acc_in,
    acc_out,
    grad_agg,
):
    def pack(at, size, row, value):
        value = value.astype(BF16)
        for j in range(4):
            onto = pl.ds(at + j * size + row, value.shape[0])
            packed[onto] = value[:, j * LANES : (j + 1) * LANES]

    own = nodes[...]
    cells[...] = cell_rows(senders[...])
    w_mid = w_edge_in[pl.ds(D, D)]
    proj[pl.ds(0, OWN)] = dot(own, w_mid).astype(BF16)
    proj[pl.ds(OWN, RIM)] = dot(rim[...], w_mid).astype(BF16)
    proj[pl.ds(CELLS, RIM_PAD - RIM)] = jnp.zeros((RIM_PAD - RIM, D), BF16)
    proj[pl.ds(OWN + RIM_PAD, OWN)] = dot(own, w_edge_in[pl.ds(2 * D, D)]).astype(BF16)

    agg[...] = jnp.zeros_like(agg)
    acc_send[...] = jnp.zeros_like(acc_send)
    acc_recv[...] = jnp.zeros_like(acc_recv)
    acc_in[...] = jnp.zeros_like(acc_in)
    acc_out[...] = jnp.zeros_like(acc_out)

    def live(step):
        slot = lax.broadcasted_iota(jnp.int32, (SLOTS, 1), 0)
        return jnp.concatenate(
            [jnp.where(slot < counts[step * PER + k], 1.0, 0.0) for k in range(PER)], axis=0
        )

    def forward(step, carry):
        span = pl.ds(pl.multiple_of(step * CHUNK, CHUNK), CHUNK)
        blocks = pl.ds(step * PER, PER)
        block = edges[span]
        recv_ids = receivers[blocks]
        picks = jnp.concatenate(
            [picks_by_slot(cells[blocks], OWN + RIM_PAD), picks_by_slot(recv_ids, OWN)], axis=1
        )
        pre = dot(block, w_edge_in[pl.ds(0, D)]) + dot(picks, proj[...])
        hidden, slope = silu_parts(pre)
        hidden = hidden.astype(BF16)
        hidden_all[span] = hidden
        slope_all[span] = slope
        standard, inverse = normalize(dot(hidden, w_edge_out[...]))
        std_all[span] = standard
        inv_all[span] = inverse
        message = standard * gain_edge[...] * live(step)
        edge_out[span] = (block.astype(F32) + message).astype(BF16)
        agg[...] += dot(picks_by_row(recv_ids, OWN), message.astype(BF16))
        return carry

    lax.fori_loop(0, STEPS, forward, 0)

    sums = agg[...].astype(BF16)
    node_pre = dot(own, w_node_in[pl.ds(0, D)]) + dot(sums, w_node_in[pl.ds(D, D)])
    node_hidden, node_slope = silu_parts(node_pre)
    node_hidden = node_hidden.astype(BF16)
    node_std, node_inv = normalize(dot(node_hidden, w_node_out[...]))
    node_out[...] = (own.astype(F32) + node_std * gain_node[...]).astype(BF16)
    upstream = cotangent[...]
    gain_sum_node = jnp.sum(upstream * node_std, 0, keepdims=True)
    grad_mlp = norm_backward(upstream * gain_node[...], node_std, node_inv).astype(BF16)
    pack(AT_NODE_OUT, D, 0, dot_at(node_hidden, grad_mlp))
    grad_node_pre = (dot_bt(grad_mlp, w_node_out[...]) * node_slope).astype(BF16)
    pack(AT_NODE_IN, 2 * D, 0, dot_at(own, grad_node_pre))
    pack(AT_NODE_IN, 2 * D, D, dot_at(sums, grad_node_pre))
    base[...] = upstream + dot_bt(grad_node_pre, w_node_in[pl.ds(0, D)])
    grad_agg[...] = dot_bt(grad_node_pre, w_node_in[pl.ds(D, D)]).astype(BF16)

    def backward(step, gain_sum):
        span = pl.ds(pl.multiple_of(step * CHUNK, CHUNK), CHUNK)
        blocks = pl.ds(step * PER, PER)
        recv_ids = receivers[blocks]
        standard = std_all[span]
        incoming = dot(picks_by_slot(recv_ids, OWN), grad_agg[...]) * live(step)
        gain_sum = gain_sum + jnp.sum(incoming * standard, 0, keepdims=True)
        grad_norm = norm_backward(incoming * gain_edge[...], standard, inv_all[span]).astype(BF16)
        acc_out[...] += dot_at(hidden_all[span], grad_norm)
        grad_pre = (dot_bt(grad_norm, w_edge_out[...]) * slope_all[span]).astype(BF16)
        acc_in[...] += dot_at(edges[span], grad_pre)
        edge_grad[span] = dot_bt(grad_pre, w_edge_in[pl.ds(0, D)]).astype(BF16)
        acc_send[...] += dot(picks_by_row(cells[blocks], CELLS), grad_pre)
        acc_recv[...] += dot(picks_by_row(recv_ids, OWN), grad_pre)
        return gain_sum

    gain_sum_edge = lax.fori_loop(0, STEPS, backward, jnp.zeros((1, D), F32))
    tail = [v[:, j * LANES : (j + 1) * LANES] for v in (gain_sum_edge, gain_sum_node) for j in range(4)]
    tail = jnp.concatenate(tail + [jnp.zeros((PACKED - AT_GAINS - 8, LANES), F32)], axis=0)
    packed[pl.ds(AT_GAINS, PACKED - AT_GAINS)] = tail.astype(BF16)
    pack(AT_EDGE_OUT, D, 0, acc_out[...])
    pack(AT_EDGE_IN, 3 * D, 0, acc_in[...])
    by_send = acc_send[...].astype(BF16)
    by_recv = acc_recv[...].astype(BF16)
    pack(AT_EDGE_IN, 3 * D, D, dot_at(own, by_send[:OWN]) + dot_at(rim[...], by_send[OWN:]))
    pack(AT_EDGE_IN, 3 * D, 2 * D, dot_at(own, by_recv))
    rim_grad[...] = dot_bt(by_send[OWN:], w_mid).astype(BF16)
    base[...] += dot_bt(by_send[:OWN], w_mid) + dot_bt(by_recv, w_edge_in[pl.ds(2 * D, D)])


def local(counts, *rest):
    shapes = [
        ((OWN, D), BF16),
        ((EDGES, D), BF16),
        ((EDGES, D), BF16),
        ((OWN, D), F32),
        ((RIM, D), BF16),
        ((PACKED, LANES), BF16),
    ]
    scratch = [
        ((TABLE, D), BF16),
        ((BLOCKS, SLOTS), jnp.int32),
        ((EDGES, D), BF16),
        ((EDGES, D), F32),
        ((EDGES, D), F32),
        ((EDGES, 1), F32),
        ((OWN, D), F32),
        ((CELLS, D), F32),
        ((OWN, D), F32),
        ((D, D), F32),
        ((D, D), F32),
        ((OWN, D), BF16),
    ]
    return pl.pallas_call(
        local_kernel,
        out_shape=[jax.ShapeDtypeStruct(s, t) for s, t in shapes],
        in_specs=[pl.BlockSpec(memory_space=pltpu.SMEM)] + whole(len(rest)),
        out_specs=whole(len(shapes)),
        scratch_shapes=[pltpu.VMEM(s, t) for s, t in scratch],
        compiler_params=pltpu.CompilerParams(vmem_limit_bytes=VMEM_LIMIT),
        name="local",
    )(counts, *rest)


def shards(
    nodes,
    edges,
    senders,
    receivers,
    counts,
    cotangent,
    w_edge_in,
    w_edge_out,
    w_node_in,
    w_node_out,
    gain_edge,
    gain_node,
):
    own = nodes.reshape(OWN, D)
    rim = halo(own)
    node_out, edge_out, edge_grad, base, rim_grad, packed = local(
        counts.reshape(BLOCKS),
        own,
        rim,
        edges.reshape(EDGES, D),
        senders.reshape(BLOCKS, SLOTS),
        receivers.reshape(BLOCKS, SLOTS),
        cotangent.reshape(OWN, D),
        w_edge_in,
        w_edge_out,
        w_node_in,
        w_node_out,
        gain_edge.reshape(1, D),
        gain_node.reshape(1, D),
    )
    total, rim_in = combine(packed, rim_grad)
    node_grad, *summed, gains = finish(total, rim_in, base)
    return (
        node_out.reshape(nodes.shape),
        edge_out.reshape(edges.shape),
        node_grad.reshape(nodes.shape),
        edge_grad.reshape(edges.shape),
        *summed,
        gains[0],
        gains[1],
    )


def solution(mesh):
    in_specs = (
        P("lat", "lon", None),
        P("lat", "lon", None, None, None),
        P("lat", "lon", None, None),
        P("lat", "lon", None, None),
        P("lat", "lon", None),
        P("lat", "lon", None),
        P(),
        P(),
        P(),
        P(),
        P(),
        P(),
    )
    out_specs = (
        P("lat", "lon", None),
        P("lat", "lon", None, None, None),
        P("lat", "lon", None),
        P("lat", "lon", None, None, None),
        P(),
        P(),
        P(),
        P(),
        P(),
        P(),
    )
    return jax.shard_map(shards, mesh=mesh, in_specs=in_specs, out_specs=out_specs, check_vma=False)
```

```python
import functools

import jax
import jax.numpy as jnp
from jax import lax
from jax.experimental import pallas as pl
from jax.experimental.pallas import tpu as pltpu
from jax.sharding import PartitionSpec as P

EPS = 1e-05
D = 512
ROWS = 16
COLS = 32
OWN = ROWS * COLS
RIM = 160
RIM_PAD = 256
CELLS = OWN + RIM
BLOCKS = 16
SLOTS = 128
EDGES = BLOCKS * SLOTS
CHUNK = 512
STEPS = EDGES // CHUNK
PER = CHUNK // SLOTS
TABLE = OWN + RIM_PAD + OWN
F32 = jnp.float32
BF16 = jnp.bfloat16
VMEM_LIMIT = 40 * 1024 * 1024

LANES = 128
AT_EDGE_IN = 0
AT_EDGE_OUT = AT_EDGE_IN + 4 * 3 * D
AT_NODE_IN = AT_EDGE_OUT + 4 * D
AT_NODE_OUT = AT_NODE_IN + 4 * 2 * D
AT_GAINS = AT_NODE_OUT + 4 * D
PACKED = 15360
HALF = PACKED // 2
PARTS = 3
PART = HALF // PARTS
PHASES = 3
TURN = ((0, 1, 2), (1, 2, 0), (2, 0, 1))
PIECE = (PART // 4, PART // 16, PART // 64)
FIRST = (PIECE[0] // 2, PIECE[1] // 2, 24)
HOPS = 6
DIRECT = (1, 2)
MESH = pl.DeviceIdType.MESH

ROUTES = (
    (-1, 0, 0, 32, 32),
    (1, 0, 32, 32, 0),
    (0, -1, 64, 16, 80),
    (0, 1, 80, 16, 64),
    (-1, -1, 96, 16, 144),
    (-1, 1, 112, 16, 128),
    (1, -1, 128, 16, 112),
    (1, 1, 144, 16, 96),
)


def dot(a, b):
    return lax.dot_general(a, b, (((1,), (0,)), ((), ())), preferred_element_type=F32)


def dot_bt(a, b):
    return lax.dot_general(a, b, (((1,), (1,)), ((), ())), preferred_element_type=F32)


def dot_at(a, b):
    return lax.dot_general(a, b, (((0,), (0,)), ((), ())), preferred_element_type=F32)


def rim_nodes(r):
    t = jnp.where(r < 32, r, 448 + r)
    t = jnp.where(r >= 64, (r - 64) * 32, t)
    t = jnp.where(r >= 80, (r - 80) * 32 + 31, t)
    t = jnp.where(r >= 96, -1, t)
    t = jnp.where(r == 96, 0, t)
    t = jnp.where(r == 112, 31, t)
    t = jnp.where(r == 128, 480, t)
    return jnp.where(r == 144, 511, t)


def rim_picks(rim_axis):
    shape = (RIM, OWN) if rim_axis == 0 else (OWN, RIM)
    r = lax.broadcasted_iota(jnp.int32, shape, rim_axis)
    n = lax.broadcasted_iota(jnp.int32, shape, 1 - rim_axis)
    return (rim_nodes(r) == n).astype(F32).astype(BF16)


class Rim:
    def __init__(self, send_buf, recv_buf, send_sem, recv_sem):
        self.refs = (send_buf, recv_buf, send_sem, recv_sem)
        self.lat, self.lon = lax.axis_index("lat"), lax.axis_index("lon")
        self.count, self.bands = lax.axis_size("lon"), lax.axis_size("lat")

    def present(self, step):
        return jnp.logical_and(self.lat + step >= 0, self.lat + step < self.bands)

    def target(self, step, turn):
        lon = lax.rem(self.lon + turn + self.count, self.count)
        return {"lat": self.lat + step, "lon": lon}

    def greet(self, barrier):
        for step, turn, _, _, _ in ROUTES:

            @pl.when(self.present(step))
            def _():
                pl.semaphore_signal(
                    barrier, inc=1, device_id=self.target(step, turn), device_id_type=MESH
                )

        up = (self.lat > 0).astype(jnp.int32)
        down = (self.lat < self.bands - 1).astype(jnp.int32)
        return 2 + 3 * up + 3 * down

    def copy(self, k):
        send_buf, recv_buf, send_sem, recv_sem = self.refs
        step, turn, start, rows, land = ROUTES[k]
        return pltpu.make_async_remote_copy(
            src_ref=send_buf.at[pl.ds(start, rows)],
            dst_ref=recv_buf.at[pl.ds(land, rows)],
            send_sem=send_sem.at[k],
            recv_sem=recv_sem.at[k],
            device_id=self.target(step, turn),
            device_id_type=MESH,
        )

    def start(self):
        for k, route in enumerate(ROUTES):

            @pl.when(self.present(route[0]))
            def _():
                self.copy(k).start()

    def wait(self):
        for k, route in enumerate(ROUTES):

            @pl.when(self.present(route[0]))
            def _():
                self.copy(k).wait_send()

            @pl.when(self.present(-route[0]))
            def _():
                self.copy(k).wait_recv()


def halo_kernel(nodes, out, send_buf, recv_buf, send_sem, recv_sem):
    rim = Rim(send_buf, recv_buf, send_sem, recv_sem)
    recv_buf[...] = jnp.zeros_like(recv_buf)
    send_buf[...] = dot(rim_picks(0), nodes[...]).astype(BF16)
    barrier = pltpu.get_barrier_semaphore()
    pl.semaphore_wait(barrier, rim.greet(barrier))
    rim.start()
    rim.wait()
    out[...] = recv_buf[...]


class Torus:
    def __init__(self):
        self.lat, self.lon = lax.axis_index("lat"), lax.axis_index("lon")
        self.core = lax.rem(self.lat, 2)
        x = (self.lon // 16) * 2 + self.lat // 2
        self.at = (x, lax.rem(self.lon, 4), lax.rem(self.lon // 4, 4))

    def near(self, axis, step):
        there = lax.rem(self.at[axis] + step + 4, 4)
        if axis == 0:
            lat = lax.rem(there, 2) * 2 + self.core
            return {"lat": lat, "lon": (there // 2) * 16 + lax.rem(self.lon, 16)}
        stride = 1 if axis == 1 else 4
        return {"lat": self.lat, "lon": self.lon + stride * (there - self.at[axis])}

    def partner(self):
        return {"lat": self.lat + 1 - 2 * self.core, "lon": self.lon}


def rows(start, size):
    return pl.ds(pl.multiple_of(start, 8), size)


def combine_kernel(
    packed,
    rim_grad,
    total,
    rim_out,
    rim_buf,
    from_core,
    wide0,
    wide1,
    wide2,
    thin0,
    thin1,
    thin2,
    first0,
    first1,
    first2,
    last0,
    last1,
    last2,
    direct,
    rim_send,
    rim_recv,
    core_send,
    core_recv,
    sum_send,
    sum_recv,
    share_send,
    share_recv,
    give_send,
    give_recv,
):
    torus = Torus()
    rim = Rim(rim_grad, rim_buf, rim_send, rim_recv)
    wide, thin = (wide0, wide1, wide2), (thin0, thin1, thin2)
    first, last = (first0, first1, first2), (last0, last1, last2)
    mine = torus.core * HALF
    other = HALF - mine
    sent = []

    def send(src, dst, send_sem, recv_sem, device):
        copy = pltpu.make_async_remote_copy(
            src_ref=src,
            dst_ref=dst,
            send_sem=send_sem,
            recv_sem=recv_sem,
            device_id=device,
            device_id_type=MESH,
        )
        copy.start()
        sent.append(copy)
        return copy

    rim_buf[...] = jnp.zeros_like(rim_buf)
    barrier = pltpu.get_barrier_semaphore()
    for device in [torus.near(axis, step) for axis in range(3) for step in (1, 2, 3)] + [
        torus.partner()
    ]:
        pl.semaphore_signal(barrier, inc=1, device_id=device, device_id_type=MESH)
    pl.semaphore_wait(barrier, 10 + rim.greet(barrier))

    def place(p, f):
        return torus.at[TURN[p][f]]

    def piece_row(p, f, shift):
        return lax.rem(place(p, f) + shift + 4, 4) * PIECE[f]

    from_partner = {}
    for shift in (2, 1, 3, 0):
        for p in range(PARTS):
            at = p * PART + piece_row(p, 0, shift)
            from_partner[p, shift] = send(
                packed.at[rows(other + at, PIECE[0])],
                from_core.at[rows(at, PIECE[0])],
                core_send.at[p * 4 + shift],
                core_recv.at[p * 4 + shift],
                torus.partner(),
            )

    def join_cores(p, shift):
        from_partner[p, shift].wait_recv()
        at = p * PART + piece_row(p, 0, shift)
        own = rows(at, PIECE[0])
        value = packed[rows(mine + at, PIECE[0])].astype(F32) + from_core[own].astype(F32)
        wide[0][own] = value
        if shift:
            thin[0][own] = value.astype(BF16)

    coming = {}

    def open_sum(p, f):
        if f in DIRECT:
            for shift in (2, 1, 3):
                k = (p * PHASES + f) * HOPS + shift
                coming[p, f, shift] = send(
                    thin[f].at[rows(p * 4 * PIECE[f] + piece_row(p, f, shift), PIECE[f])],
                    direct.at[f - 1, p, shift, pl.ds(0, PIECE[f])],
                    sum_send.at[k],
                    sum_recv.at[k],
                    torus.near(TURN[p][f], shift),
                )
            return
        axis, half = TURN[p][f], FIRST[f]
        rest = PIECE[f] - half
        right, left = torus.near(axis, 1), torus.near(axis, -1)
        start = p * 4 * PIECE[f]
        toward(p, f, 0, start + piece_row(p, f, 2), half, first[f], 0, right)
        toward(p, f, 1, start + piece_row(p, f, 2) + half, rest, last[f], 0, left)

    def toward(p, f, k, row, size, buf, slot, device):
        base = (p * PHASES + f) * HOPS
        coming[p, f, k] = send(
            thin[f].at[rows(row, size)],
            buf.at[p * 3 + slot],
            sum_send.at[base + k],
            sum_recv.at[base + k],
            device,
        )

    def fill_sum(p, f):
        axis, half = TURN[p][f], FIRST[f]
        rest = PIECE[f] - half
        right, left = torus.near(axis, 1), torus.near(axis, -1)
        start = p * 4 * PIECE[f]
        toward(p, f, 2, start + piece_row(p, f, 1) + half, rest, last[f], 1, right)
        toward(p, f, 3, start + piece_row(p, f, -1), half, first[f], 1, left)

    def join_sum(p, f):
        if f in DIRECT:
            return
        axis, half = TURN[p][f], FIRST[f]
        rest = PIECE[f] - half
        base = (p * PHASES + f) * HOPS
        start = p * 4 * PIECE[f]

        def go(k, row, size, buf, device):
            coming[p, f, k - 4].wait_recv()
            joined = buf[p * 3].astype(F32) + wide[f][rows(start + row, size)]
            buf[9 + p] = joined.astype(BF16)
            coming[p, f, k] = send(
                buf.at[9 + p],
                buf.at[p * 3 + 2],
                sum_send.at[base + k],
                sum_recv.at[base + k],
                device,
            )

        go(4, piece_row(p, f, 1), half, first[f], torus.near(axis, 1))
        go(5, piece_row(p, f, -1) + half, rest, last[f], torus.near(axis, -1))

    def close_sum(p, f):
        half = FIRST[f]
        rest = PIECE[f] - half
        start = p * 4 * PIECE[f] + piece_row(p, f, 0)
        if f in DIRECT:
            value = wide[f][rows(start, PIECE[f])]
            for shift in (1, 3, 2):
                coming[p, f, shift].wait_recv()
                value = value + direct[f - 1, p, shift, pl.ds(0, PIECE[f])].astype(F32)
            if f + 1 < PHASES:
                onto = pl.ds(p * PIECE[f], PIECE[f])
                wide[f + 1][onto] = value
                thin[f + 1][onto] = value.astype(BF16)
            else:
                total[rows(block_row(p, f, 0), PIECE[f])] = value.astype(BF16)
            return
        for k in (3, 2, 4, 5):
            coming[p, f, k].wait_recv()
        for offset, size, buf in ((0, half, first[f]), (half, rest, last[f])):
            value = (
                wide[f][rows(start + offset, size)]
                + buf[p * 3 + 1].astype(F32)
                + buf[p * 3 + 2].astype(F32)
            )
            if f + 1 < PHASES:
                onto = pl.ds(p * PIECE[f] + offset, size)
                wide[f + 1][onto] = value
                thin[f + 1][onto] = value.astype(BF16)
            else:
                total[rows(block_row(p, f, 0) + offset, size)] = value.astype(BF16)

    def block_row(p, f, shift):
        row = mine + p * PART + piece_row(p, f, shift)
        for g in range(f):
            row = row + piece_row(p, g, 0)
        return row

    for p in range(PARTS):
        join_cores(p, 2)
        open_sum(p, 0)
    for p in range(PARTS):
        join_cores(p, 1)
        join_cores(p, 3)
        fill_sum(p, 0)
    for p in range(PARTS):
        join_cores(p, 0)
    for f in range(PHASES):
        for p in range(PARTS):
            join_sum(p, f)
        if f == 0:
            rim.start()
        for p in range(PARTS):
            close_sum(p, f)
            if f + 1 < PHASES:
                open_sum(p, f + 1)

    def share(p, f, k, shift, offset, size, device):
        region = total.at[rows(block_row(p, f, shift) + offset, size)]
        base = (p * PHASES + f) * HOPS
        coming[p, f, k] = send(
            region, region, share_send.at[base + k], share_recv.at[base + k], device
        )

    def open_share(p, f):
        if f in DIRECT:
            for shift in (2, 1, 3):
                share(p, f, shift, 0, 0, PIECE[f], torus.near(TURN[p][f], shift))
            return
        axis, half = TURN[p][f], FIRST[f]
        rest = PIECE[f] - half
        right, left = torus.near(axis, 1), torus.near(axis, -1)
        share(p, f, 0, 0, 0, half, right)
        share(p, f, 1, 0, half, rest, left)
        share(p, f, 2, 0, half, rest, right)
        share(p, f, 3, 0, 0, half, left)

    def relay_share(p, f):
        if f in DIRECT:
            return
        axis, half = TURN[p][f], FIRST[f]
        rest = PIECE[f] - half
        coming[p, f, 0].wait_recv()
        share(p, f, 4, -1, 0, half, torus.near(axis, 1))
        coming[p, f, 1].wait_recv()
        share(p, f, 5, 1, half, rest, torus.near(axis, -1))

    given = []

    def give(p, shift, offset, size, k):
        region = total.at[rows(block_row(p, 0, shift) + offset, size)]
        slot = p * 5 + k
        given.append(
            send(region, region, give_send.at[slot], give_recv.at[slot], torus.partner())
        )

    for p in range(PARTS):
        open_share(p, PHASES - 1)
    for f in DIRECT[::-1]:
        for p in range(PARTS):
            for shift in (1, 3, 2):
                coming[p, f, shift].wait_recv()
            open_share(p, f - 1)
    for p in range(PARTS):
        give(p, 0, 0, PIECE[0], 0)
    for p in range(PARTS):
        relay_share(p, 0)
    for p in range(PARTS):
        coming[p, 0, 2].wait_recv()
        give(p, -1, 0, PIECE[0], 1)
        coming[p, 0, 3].wait_recv()
        give(p, 1, 0, PIECE[0], 2)
    for p in range(PARTS):
        coming[p, 0, 4].wait_recv()
        give(p, 2, 0, FIRST[0], 3)
        coming[p, 0, 5].wait_recv()
        give(p, 2, FIRST[0], PIECE[0] - FIRST[0], 4)
    rim.wait()
    rim_out[...] = rim_buf[...]
    for copy in given:
        copy.wait_recv()
    for copy in sent:
        copy.wait_send()


def whole(n):
    return [pl.BlockSpec(memory_space=pltpu.VMEM)] * n


def combine(packed, rim_grad):
    dma = pltpu.SemaphoreType.DMA
    hops = PARTS * PHASES * HOPS
    scratch = [pltpu.VMEM((RIM, D), BF16), pltpu.VMEM((HALF, LANES), BF16)]
    scratch += [pltpu.VMEM((PARTS * 4 * n, LANES), F32) for n in PIECE]
    scratch += [pltpu.VMEM((PARTS * 4 * n, LANES), BF16) for n in PIECE]
    scratch += [pltpu.VMEM((12, n, LANES), BF16) for n in FIRST]
    scratch += [pltpu.VMEM((12, m - n, LANES), BF16) for m, n in zip(PIECE, FIRST)]
    scratch += [pltpu.VMEM((2, PARTS, 4, PIECE[1], LANES), BF16)]
    scratch += [dma((n,)) for n in (8, 8, 12, 12, hops, hops, hops, hops, 15, 15)]
    return pl.pallas_call(
        combine_kernel,
        out_shape=[
            jax.ShapeDtypeStruct((PACKED, LANES), BF16),
            jax.ShapeDtypeStruct((RIM, D), BF16),
        ],
        in_specs=whole(2),
        out_specs=whole(2),
        scratch_shapes=scratch,
        compiler_params=pltpu.CompilerParams(
            collective_id=1, has_side_effects=True, vmem_limit_bytes=24 * 1024 * 1024
        ),
        name="combine",
    )(packed, rim_grad)


def finish_kernel(
    total,
    rim_in,
    base,
    node_grad,
    g_edge_in,
    g_edge_out,
    g_node_in,
    g_node_out,
    gain_edge,
    gain_node,
    sems,
):
    copies = []
    for out, at in (
        (g_edge_in, AT_EDGE_IN),
        (g_edge_out, AT_EDGE_OUT),
        (g_node_in, AT_NODE_IN),
        (g_node_out, AT_NODE_OUT),
    ):
        size = out.shape[0]
        for j in range(4):
            copies.append(
                pltpu.make_async_copy(
                    total.at[pl.ds(at + j * size, size)],
                    out.at[:, pl.ds(j * LANES, LANES)],
                    sems.at[len(copies)],
                )
            )
            copies[-1].start()
    tail = total[pl.ds(AT_GAINS, 16)].astype(F32)
    for j in range(4):
        gain_edge[:, pl.ds(j * LANES, LANES)] = tail[j : j + 1]
        gain_node[:, pl.ds(j * LANES, LANES)] = tail[4 + j : 5 + j]
    node_grad[...] = (base[...] + dot(rim_picks(1), rim_in[...])).astype(BF16)
    for copy in copies:
        copy.wait()


def finish(total, rim_in, base):
    shapes = [
        ((OWN, D), BF16),
        ((3 * D, D), BF16),
        ((D, D), BF16),
        ((2 * D, D), BF16),
        ((D, D), BF16),
        ((1, D), F32),
        ((1, D), F32),
    ]
    anywhere = [pl.BlockSpec(memory_space=pl.ANY)] * 4
    return pl.pallas_call(
        finish_kernel,
        out_shape=[jax.ShapeDtypeStruct(s, t) for s, t in shapes],
        in_specs=whole(3),
        out_specs=whole(1) + anywhere + whole(2),
        scratch_shapes=[pltpu.SemaphoreType.DMA((16,))],
        compiler_params=pltpu.CompilerParams(vmem_limit_bytes=16 * 1024 * 1024),
        name="finish",
    )(total, rim_in, base)


RIM_SCRATCH = [
    pltpu.VMEM((RIM, D), BF16),
    pltpu.VMEM((RIM, D), BF16),
    pltpu.SemaphoreType.DMA((len(ROUTES),)),
    pltpu.SemaphoreType.DMA((len(ROUTES),)),
]


def halo(nodes):
    return pl.pallas_call(
        halo_kernel,
        out_shape=jax.ShapeDtypeStruct((RIM, D), BF16),
        in_specs=whole(1),
        out_specs=whole(1)[0],
        scratch_shapes=RIM_SCRATCH,
        compiler_params=pltpu.CompilerParams(
            collective_id=0, has_side_effects=True, vmem_limit_bytes=8 * 1024 * 1024
        ),
        cost_estimate=pl.CostEstimate(flops=6 * 10**9, bytes_accessed=2**20, transcendentals=0),
        name="halo",
    )(nodes)


def normalize(values):
    average = jnp.mean(values, -1, keepdims=True)
    centred = values - average
    spread = jnp.mean(centred * centred, -1, keepdims=True)
    inverse = lax.rsqrt(spread + EPS)
    return centred * inverse, inverse


def norm_backward(scaled, standard, inverse):
    return inverse * (
        scaled
        - jnp.mean(scaled, -1, keepdims=True)
        - standard * jnp.mean(scaled * standard, -1, keepdims=True)
    )


def silu_parts(values):
    logistic = 1.0 / (1.0 + jnp.exp(-values))
    hidden = values * logistic
    return hidden, logistic * (1.0 + values * (1.0 - logistic))


def cell_rows(senders):
    row = (senders * 1928) >> 16
    col = senders - row * 34
    left, right = col == 0, col == 33
    top, bottom = row == 0, row == 17
    place = (row - 1) * 32 + col - 1
    place = jnp.where(top, OWN + col - 1, place)
    place = jnp.where(bottom, OWN + 32 + col - 1, place)
    place = jnp.where(left, OWN + 64 + row - 1, place)
    place = jnp.where(right, OWN + 80 + row - 1, place)
    place = jnp.where(jnp.logical_and(top, left), OWN + 96, place)
    place = jnp.where(jnp.logical_and(top, right), OWN + 112, place)
    place = jnp.where(jnp.logical_and(bottom, left), OWN + 128, place)
    return jnp.where(jnp.logical_and(bottom, right), OWN + 144, place)


def one_hot(mask):
    return jnp.where(mask, 1.0, 0.0).astype(BF16)


def picks_by_slot(ids, width):
    parts = []
    for k in range(PER):
        column = jnp.broadcast_to(ids[k : k + 1], (SLOTS, SLOTS)).T
        lanes = lax.broadcasted_iota(jnp.int32, (SLOTS, SLOTS), 1)
        parts.append(
            jnp.concatenate([one_hot(column == lanes + s) for s in range(0, width, SLOTS)], axis=1)
        )
    return jnp.concatenate(parts, axis=0)


def picks_by_row(ids, height):
    rows = lax.broadcasted_iota(jnp.int32, (height, SLOTS), 0)
    return jnp.concatenate([one_hot(rows == ids[k : k + 1]) for k in range(PER)], axis=1)


def local_kernel(
    counts,
    nodes,
    rim,
    edges,
    senders,
    receivers,
    cotangent,
    w_edge_in,
    w_edge_out,
    w_node_in,
    w_node_out,
    gain_edge,
    gain_node,
    node_out_far,
    edge_out_far,
    edge_grad_far,
    base,
    rim_grad,
    packed,
    node_out,
    edge_out,
    edge_grad,
    sems,
    proj,
    cells,
    hidden_all,
    slope_all,
    std_all,
    inv_all,
    agg,
    acc_send,
    acc_recv,
    acc_in,
    acc_out,
    grad_agg,
):
    def chunk_out(step, near, far, at):
        span = rows(step * CHUNK, CHUNK)
        return pltpu.make_async_copy(near.at[span], far.at[span], sems.at[at + step])

    node_copy = pltpu.make_async_copy(node_out, node_out_far, sems.at[2 * STEPS])

    def pack(at, size, row, value):
        value = value.astype(BF16)
        for j in range(4):
            onto = pl.ds(at + j * size + row, value.shape[0])
            packed[onto] = value[:, j * LANES : (j + 1) * LANES]

    own = nodes[...]
    cells[...] = cell_rows(senders[...])
    w_mid = w_edge_in[pl.ds(D, D)]
    proj[pl.ds(0, OWN)] = dot(own, w_mid).astype(BF16)
    proj[pl.ds(OWN, RIM)] = dot(rim[...], w_mid).astype(BF16)
    proj[pl.ds(CELLS, RIM_PAD - RIM)] = jnp.zeros((RIM_PAD - RIM, D), BF16)
    proj[pl.ds(OWN + RIM_PAD, OWN)] = dot(own, w_edge_in[pl.ds(2 * D, D)]).astype(BF16)

    agg[...] = jnp.zeros_like(agg)
    acc_send[...] = jnp.zeros_like(acc_send)
    acc_recv[...] = jnp.zeros_like(acc_recv)
    acc_in[...] = jnp.zeros_like(acc_in)
    acc_out[...] = jnp.zeros_like(acc_out)

    def live(step):
        slot = lax.broadcasted_iota(jnp.int32, (SLOTS, 1), 0)
        return jnp.concatenate(
            [jnp.where(slot < counts[step * PER + k], 1.0, 0.0) for k in range(PER)], axis=0
        )

    def forward(step, carry):
        span = pl.ds(pl.multiple_of(step * CHUNK, CHUNK), CHUNK)
        blocks = pl.ds(step * PER, PER)
        block = edges[span]
        recv_ids = receivers[blocks]
        picks = jnp.concatenate(
            [picks_by_slot(cells[blocks], OWN + RIM_PAD), picks_by_slot(recv_ids, OWN)], axis=1
        )
        pre = dot(block, w_edge_in[pl.ds(0, D)]) + dot(picks, proj[...])
        hidden, slope = silu_parts(pre)
        hidden = hidden.astype(BF16)
        hidden_all[span] = hidden
        slope_all[span] = slope
        standard, inverse = normalize(dot(hidden, w_edge_out[...]))
        std_all[span] = standard
        inv_all[span] = inverse
        message = standard * gain_edge[...] * live(step)
        edge_out[span] = (block.astype(F32) + message).astype(BF16)
        chunk_out(step, edge_out, edge_out_far, 0).start()
        agg[...] += dot(picks_by_row(recv_ids, OWN), message.astype(BF16))
        return carry

    lax.fori_loop(0, STEPS, forward, 0)

    sums = agg[...].astype(BF16)
    node_pre = dot(own, w_node_in[pl.ds(0, D)]) + dot(sums, w_node_in[pl.ds(D, D)])
    node_hidden, node_slope = silu_parts(node_pre)
    node_hidden = node_hidden.astype(BF16)
    node_std, node_inv = normalize(dot(node_hidden, w_node_out[...]))
    node_out[...] = (own.astype(F32) + node_std * gain_node[...]).astype(BF16)
    node_copy.start()
    upstream = cotangent[...]
    gain_sum_node = jnp.sum(upstream * node_std, 0, keepdims=True)
    grad_mlp = norm_backward(upstream * gain_node[...], node_std, node_inv).astype(BF16)
    pack(AT_NODE_OUT, D, 0, dot_at(node_hidden, grad_mlp))
    grad_node_pre = (dot_bt(grad_mlp, w_node_out[...]) * node_slope).astype(BF16)
    pack(AT_NODE_IN, 2 * D, 0, dot_at(own, grad_node_pre))
    pack(AT_NODE_IN, 2 * D, D, dot_at(sums, grad_node_pre))
    base[...] = upstream + dot_bt(grad_node_pre, w_node_in[pl.ds(0, D)])
    grad_agg[...] = dot_bt(grad_node_pre, w_node_in[pl.ds(D, D)]).astype(BF16)

    def backward(step, gain_sum):
        span = pl.ds(pl.multiple_of(step * CHUNK, CHUNK), CHUNK)
        blocks = pl.ds(step * PER, PER)
        recv_ids = receivers[blocks]
        standard = std_all[span]
        incoming = dot(picks_by_slot(recv_ids, OWN), grad_agg[...]) * live(step)
        gain_sum = gain_sum + jnp.sum(incoming * standard, 0, keepdims=True)
        grad_norm = norm_backward(incoming * gain_edge[...], standard, inv_all[span]).astype(BF16)
        acc_out[...] += dot_at(hidden_all[span], grad_norm)
        grad_pre = (dot_bt(grad_norm, w_edge_out[...]) * slope_all[span]).astype(BF16)
        acc_in[...] += dot_at(edges[span], grad_pre)
        edge_grad[span] = dot_bt(grad_pre, w_edge_in[pl.ds(0, D)]).astype(BF16)
        chunk_out(step, edge_grad, edge_grad_far, STEPS).start()
        acc_send[...] += dot(picks_by_row(cells[blocks], CELLS), grad_pre)
        acc_recv[...] += dot(picks_by_row(recv_ids, OWN), grad_pre)
        return gain_sum

    gain_sum_edge = lax.fori_loop(0, STEPS, backward, jnp.zeros((1, D), F32))
    tail = [v[:, j * LANES : (j + 1) * LANES] for v in (gain_sum_edge, gain_sum_node) for j in range(4)]
    tail = jnp.concatenate(tail + [jnp.zeros((PACKED - AT_GAINS - 8, LANES), F32)], axis=0)
    packed[pl.ds(AT_GAINS, PACKED - AT_GAINS)] = tail.astype(BF16)
    pack(AT_EDGE_OUT, D, 0, acc_out[...])
    pack(AT_EDGE_IN, 3 * D, 0, acc_in[...])
    by_send = acc_send[...].astype(BF16)
    by_recv = acc_recv[...].astype(BF16)
    pack(AT_EDGE_IN, 3 * D, D, dot_at(own, by_send[:OWN]) + dot_at(rim[...], by_send[OWN:]))
    pack(AT_EDGE_IN, 3 * D, 2 * D, dot_at(own, by_recv))
    rim_grad[...] = dot_bt(by_send[OWN:], w_mid).astype(BF16)
    base[...] += dot_bt(by_send[:OWN], w_mid) + dot_bt(by_recv, w_edge_in[pl.ds(2 * D, D)])
    node_copy.wait()
    for step in range(STEPS):
        chunk_out(step, edge_out, edge_out_far, 0).wait()
        chunk_out(step, edge_grad, edge_grad_far, STEPS).wait()


def local(counts, *rest):
    shapes = [
        ((OWN, D), BF16),
        ((EDGES, D), BF16),
        ((EDGES, D), BF16),
        ((OWN, D), F32),
        ((RIM, D), BF16),
        ((PACKED, LANES), BF16),
    ]
    scratch = [
        ((TABLE, D), BF16),
        ((BLOCKS, SLOTS), jnp.int32),
        ((EDGES, D), BF16),
        ((EDGES, D), F32),
        ((EDGES, D), F32),
        ((EDGES, 1), F32),
        ((OWN, D), F32),
        ((CELLS, D), F32),
        ((OWN, D), F32),
        ((D, D), F32),
        ((D, D), F32),
        ((OWN, D), BF16),
    ]
    return pl.pallas_call(
        local_kernel,
        out_shape=[jax.ShapeDtypeStruct(s, t) for s, t in shapes],
        in_specs=[pl.BlockSpec(memory_space=pltpu.SMEM)] + whole(len(rest)),
        out_specs=[pl.BlockSpec(memory_space=pl.ANY)] * 3 + whole(3),
        scratch_shapes=[pltpu.VMEM(s, t) for s, t in shapes[:3]]
        + [pltpu.SemaphoreType.DMA((2 * STEPS + 1,))]
        + [pltpu.VMEM(s, t) for s, t in scratch],
        compiler_params=pltpu.CompilerParams(vmem_limit_bytes=VMEM_LIMIT),
        name="local",
    )(counts, *rest)


def shards(
    nodes,
    edges,
    senders,
    receivers,
    counts,
    cotangent,
    w_edge_in,
    w_edge_out,
    w_node_in,
    w_node_out,
    gain_edge,
    gain_node,
):
    own = nodes.reshape(OWN, D)
    rim = halo(own)
    node_out, edge_out, edge_grad, base, rim_grad, packed = local(
        counts.reshape(BLOCKS),
        own,
        rim,
        edges.reshape(EDGES, D),
        senders.reshape(BLOCKS, SLOTS),
        receivers.reshape(BLOCKS, SLOTS),
        cotangent.reshape(OWN, D),
        w_edge_in,
        w_edge_out,
        w_node_in,
        w_node_out,
        gain_edge.reshape(1, D),
        gain_node.reshape(1, D),
    )
    total, rim_in = combine(packed, rim_grad)
    node_grad, *summed, gain_sum_edge, gain_sum_node = finish(total, rim_in, base)
    return (
        node_out.reshape(nodes.shape),
        edge_out.reshape(edges.shape),
        node_grad.reshape(nodes.shape),
        edge_grad.reshape(edges.shape),
        *summed,
        gain_sum_edge.reshape(D),
        gain_sum_node.reshape(D),
    )


def solution(mesh):
    in_specs = (
        P("lat", "lon", None),
        P("lat", "lon", None, None, None),
        P("lat", "lon", None, None),
        P("lat", "lon", None, None),
        P("lat", "lon", None),
        P("lat", "lon", None),
        P(),
        P(),
        P(),
        P(),
        P(),
        P(),
    )
    out_specs = (
        P("lat", "lon", None),
        P("lat", "lon", None, None, None),
        P("lat", "lon", None),
        P("lat", "lon", None, None, None),
        P(),
        P(),
        P(),
        P(),
        P(),
        P(),
    )
    return jax.shard_map(shards, mesh=mesh, in_specs=in_specs, out_specs=out_specs, check_vma=False)
```

```python
import functools

import jax
import jax.numpy as jnp
from jax import lax
from jax.experimental import pallas as pl
from jax.experimental.pallas import tpu as pltpu
from jax.sharding import PartitionSpec as P

EPS = 1e-05
D = 512
ROWS = 16
COLS = 32
OWN = ROWS * COLS
RIM = 160
RIM_PAD = 256
CELLS = OWN + RIM
BLOCKS = 16
SLOTS = 128
EDGES = BLOCKS * SLOTS
CHUNK = 512
STEPS = EDGES // CHUNK
PER = CHUNK // SLOTS
TABLE = OWN + RIM_PAD + OWN
F32 = jnp.float32
BF16 = jnp.bfloat16
VMEM_LIMIT = 40 * 1024 * 1024

LANES = 128
AT_EDGE_IN = 0
AT_EDGE_OUT = AT_EDGE_IN + 4 * 3 * D
AT_NODE_IN = AT_EDGE_OUT + 4 * D
AT_NODE_OUT = AT_NODE_IN + 4 * 2 * D
AT_GAINS = AT_NODE_OUT + 4 * D
PACKED = 15360
HALF = PACKED // 2
PARTS = 3
PART = HALF // PARTS
PHASES = 3
TURN = ((0, 1, 2), (1, 2, 0), (2, 0, 1))
PIECE = (PART // 4, PART // 16, PART // 64)
FIRST = (PIECE[0] // 2, PIECE[1] // 2, 24)
HOPS = 6
DIRECT = (1, 2)
MESH = pl.DeviceIdType.MESH

ROUTES = (
    (-1, 0, 0, 32, 32),
    (1, 0, 32, 32, 0),
    (0, -1, 64, 16, 80),
    (0, 1, 80, 16, 64),
    (-1, -1, 96, 16, 144),
    (-1, 1, 112, 16, 128),
    (1, -1, 128, 16, 112),
    (1, 1, 144, 16, 96),
)


def dot(a, b):
    return lax.dot_general(a, b, (((1,), (0,)), ((), ())), preferred_element_type=F32)


def dot_bt(a, b):
    return lax.dot_general(a, b, (((1,), (1,)), ((), ())), preferred_element_type=F32)


def dot_at(a, b):
    return lax.dot_general(a, b, (((0,), (0,)), ((), ())), preferred_element_type=F32)


def rim_nodes(r):
    t = jnp.where(r < 32, r, 448 + r)
    t = jnp.where(r >= 64, (r - 64) * 32, t)
    t = jnp.where(r >= 80, (r - 80) * 32 + 31, t)
    t = jnp.where(r >= 96, -1, t)
    t = jnp.where(r == 96, 0, t)
    t = jnp.where(r == 112, 31, t)
    t = jnp.where(r == 128, 480, t)
    return jnp.where(r == 144, 511, t)


def rim_picks(rim_axis):
    shape = (RIM, OWN) if rim_axis == 0 else (OWN, RIM)
    r = lax.broadcasted_iota(jnp.int32, shape, rim_axis)
    n = lax.broadcasted_iota(jnp.int32, shape, 1 - rim_axis)
    return (rim_nodes(r) == n).astype(F32).astype(BF16)


class Rim:
    def __init__(self, send_buf, recv_buf, send_sem, recv_sem):
        self.refs = (send_buf, recv_buf, send_sem, recv_sem)
        self.lat, self.lon = lax.axis_index("lat"), lax.axis_index("lon")
        self.count, self.bands = lax.axis_size("lon"), lax.axis_size("lat")

    def present(self, step):
        return jnp.logical_and(self.lat + step >= 0, self.lat + step < self.bands)

    def target(self, step, turn):
        lon = lax.rem(self.lon + turn + self.count, self.count)
        return {"lat": self.lat + step, "lon": lon}

    def greet(self, barrier):
        for step, turn, _, _, _ in ROUTES:

            @pl.when(self.present(step))
            def _():
                pl.semaphore_signal(
                    barrier, inc=1, device_id=self.target(step, turn), device_id_type=MESH
                )

        up = (self.lat > 0).astype(jnp.int32)
        down = (self.lat < self.bands - 1).astype(jnp.int32)
        return 2 + 3 * up + 3 * down

    def copy(self, k):
        send_buf, recv_buf, send_sem, recv_sem = self.refs
        step, turn, start, rows, land = ROUTES[k]
        return pltpu.make_async_remote_copy(
            src_ref=send_buf.at[pl.ds(start, rows)],
            dst_ref=recv_buf.at[pl.ds(land, rows)],
            send_sem=send_sem.at[k],
            recv_sem=recv_sem.at[k],
            device_id=self.target(step, turn),
            device_id_type=MESH,
        )

    def start(self):
        for k, route in enumerate(ROUTES):

            @pl.when(self.present(route[0]))
            def _():
                self.copy(k).start()

    def wait(self):
        for k, route in enumerate(ROUTES):

            @pl.when(self.present(route[0]))
            def _():
                self.copy(k).wait_send()

            @pl.when(self.present(-route[0]))
            def _():
                self.copy(k).wait_recv()


def halo_kernel(nodes, out, send_buf, recv_buf, send_sem, recv_sem):
    rim = Rim(send_buf, recv_buf, send_sem, recv_sem)
    recv_buf[...] = jnp.zeros_like(recv_buf)
    send_buf[...] = dot(rim_picks(0), nodes[...]).astype(BF16)
    barrier = pltpu.get_barrier_semaphore()
    pl.semaphore_wait(barrier, rim.greet(barrier))
    rim.start()
    rim.wait()
    out[...] = recv_buf[...]


class Torus:
    def __init__(self):
        self.lat, self.lon = lax.axis_index("lat"), lax.axis_index("lon")
        self.core = lax.rem(self.lat, 2)
        x = (self.lon // 16) * 2 + self.lat // 2
        self.at = (x, lax.rem(self.lon, 4), lax.rem(self.lon // 4, 4))

    def near(self, axis, step):
        there = lax.rem(self.at[axis] + step + 4, 4)
        if axis == 0:
            lat = lax.rem(there, 2) * 2 + self.core
            return {"lat": lat, "lon": (there // 2) * 16 + lax.rem(self.lon, 16)}
        stride = 1 if axis == 1 else 4
        return {"lat": self.lat, "lon": self.lon + stride * (there - self.at[axis])}

    def partner(self):
        return {"lat": self.lat + 1 - 2 * self.core, "lon": self.lon}


def rows(start, size):
    return pl.ds(pl.multiple_of(start, 8), size)


def combine_kernel(
    packed,
    rim_grad,
    total,
    rim_out,
    rim_buf,
    from_core,
    wide0,
    wide1,
    wide2,
    thin0,
    thin1,
    thin2,
    first0,
    first1,
    first2,
    last0,
    last1,
    last2,
    direct,
    rim_send,
    rim_recv,
    core_send,
    core_recv,
    sum_send,
    sum_recv,
    share_send,
    share_recv,
    give_send,
    give_recv,
):
    torus = Torus()
    rim = Rim(rim_grad, rim_buf, rim_send, rim_recv)
    wide, thin = (wide0, wide1, wide2), (thin0, thin1, thin2)
    first, last = (first0, first1, first2), (last0, last1, last2)
    mine = torus.core * HALF
    other = HALF - mine
    sent = []

    def send(src, dst, send_sem, recv_sem, device):
        copy = pltpu.make_async_remote_copy(
            src_ref=src,
            dst_ref=dst,
            send_sem=send_sem,
            recv_sem=recv_sem,
            device_id=device,
            device_id_type=MESH,
        )
        copy.start()
        sent.append(copy)
        return copy

    rim_buf[...] = jnp.zeros_like(rim_buf)
    barrier = pltpu.get_barrier_semaphore()
    for device in [torus.near(axis, step) for axis in range(3) for step in (1, 2, 3)] + [
        torus.partner()
    ]:
        pl.semaphore_signal(barrier, inc=1, device_id=device, device_id_type=MESH)
    pl.semaphore_wait(barrier, 10 + rim.greet(barrier))

    def place(p, f):
        return torus.at[TURN[p][f]]

    def piece_row(p, f, shift):
        return lax.rem(place(p, f) + shift + 4, 4) * PIECE[f]

    from_partner = {}
    for shift in (2, 1, 3, 0):
        for p in range(PARTS):
            at = p * PART + piece_row(p, 0, shift)
            from_partner[p, shift] = send(
                packed.at[rows(other + at, PIECE[0])],
                from_core.at[rows(at, PIECE[0])],
                core_send.at[p * 4 + shift],
                core_recv.at[p * 4 + shift],
                torus.partner(),
            )

    def join_cores(p, shift):
        from_partner[p, shift].wait_recv()
        at = p * PART + piece_row(p, 0, shift)
        own = rows(at, PIECE[0])
        value = packed[rows(mine + at, PIECE[0])].astype(F32) + from_core[own].astype(F32)
        wide[0][own] = value
        if shift:
            thin[0][own] = value.astype(BF16)

    coming = {}

    def open_sum(p, f):
        if f in DIRECT:
            for shift in (2, 1, 3):
                k = (p * PHASES + f) * HOPS + shift
                coming[p, f, shift] = send(
                    thin[f].at[rows(p * 4 * PIECE[f] + piece_row(p, f, shift), PIECE[f])],
                    direct.at[f - 1, p, shift, pl.ds(0, PIECE[f])],
                    sum_send.at[k],
                    sum_recv.at[k],
                    torus.near(TURN[p][f], shift),
                )
            return
        axis, half = TURN[p][f], FIRST[f]
        rest = PIECE[f] - half
        right, left = torus.near(axis, 1), torus.near(axis, -1)
        start = p * 4 * PIECE[f]
        toward(p, f, 0, start + piece_row(p, f, 2), half, first[f], 0, right)
        toward(p, f, 1, start + piece_row(p, f, 2) + half, rest, last[f], 0, left)

    def toward(p, f, k, row, size, buf, slot, device):
        base = (p * PHASES + f) * HOPS
        coming[p, f, k] = send(
            thin[f].at[rows(row, size)],
            buf.at[p * 3 + slot],
            sum_send.at[base + k],
            sum_recv.at[base + k],
            device,
        )

    def fill_sum(p, f):
        axis, half = TURN[p][f], FIRST[f]
        rest = PIECE[f] - half
        right, left = torus.near(axis, 1), torus.near(axis, -1)
        start = p * 4 * PIECE[f]
        toward(p, f, 2, start + piece_row(p, f, 1) + half, rest, last[f], 1, right)
        toward(p, f, 3, start + piece_row(p, f, -1), half, first[f], 1, left)

    def join_sum(p, f):
        if f in DIRECT:
            return
        axis, half = TURN[p][f], FIRST[f]
        rest = PIECE[f] - half
        base = (p * PHASES + f) * HOPS
        start = p * 4 * PIECE[f]

        def go(k, row, size, buf, device):
            coming[p, f, k - 4].wait_recv()
            joined = buf[p * 3].astype(F32) + wide[f][rows(start + row, size)]
            buf[9 + p] = joined.astype(BF16)
            coming[p, f, k] = send(
                buf.at[9 + p],
                buf.at[p * 3 + 2],
                sum_send.at[base + k],
                sum_recv.at[base + k],
                device,
            )

        go(4, piece_row(p, f, 1), half, first[f], torus.near(axis, 1))
        go(5, piece_row(p, f, -1) + half, rest, last[f], torus.near(axis, -1))

    def close_sum(p, f):
        half = FIRST[f]
        rest = PIECE[f] - half
        start = p * 4 * PIECE[f] + piece_row(p, f, 0)
        if f in DIRECT:
            value = wide[f][rows(start, PIECE[f])]
            for shift in (1, 3, 2):
                coming[p, f, shift].wait_recv()
                value = value + direct[f - 1, p, shift, pl.ds(0, PIECE[f])].astype(F32)
            if f + 1 < PHASES:
                onto = pl.ds(p * PIECE[f], PIECE[f])
                wide[f + 1][onto] = value
                thin[f + 1][onto] = value.astype(BF16)
            else:
                total[rows(block_row(p, f, 0), PIECE[f])] = value.astype(BF16)
            return
        for k in (3, 2, 4, 5):
            coming[p, f, k].wait_recv()
        for offset, size, buf in ((0, half, first[f]), (half, rest, last[f])):
            value = (
                wide[f][rows(start + offset, size)]
                + buf[p * 3 + 1].astype(F32)
                + buf[p * 3 + 2].astype(F32)
            )
            if f + 1 < PHASES:
                onto = pl.ds(p * PIECE[f] + offset, size)
                wide[f + 1][onto] = value
                thin[f + 1][onto] = value.astype(BF16)
            else:
                total[rows(block_row(p, f, 0) + offset, size)] = value.astype(BF16)

    def block_row(p, f, shift):
        row = mine + p * PART + piece_row(p, f, shift)
        for g in range(f):
            row = row + piece_row(p, g, 0)
        return row

    for p in range(PARTS):
        join_cores(p, 2)
        open_sum(p, 0)
    for p in range(PARTS):
        join_cores(p, 1)
        join_cores(p, 3)
        fill_sum(p, 0)
    for p in range(PARTS):
        join_cores(p, 0)
    for f in range(PHASES):
        for p in range(PARTS):
            join_sum(p, f)
        if f == 0:
            rim.start()
        for p in range(PARTS):
            close_sum(p, f)
            if f + 1 < PHASES:
                open_sum(p, f + 1)

    def share(p, f, k, shift, offset, size, device):
        region = total.at[rows(block_row(p, f, shift) + offset, size)]
        base = (p * PHASES + f) * HOPS
        coming[p, f, k] = send(
            region, region, share_send.at[base + k], share_recv.at[base + k], device
        )

    def open_share(p, f):
        if f in DIRECT:
            for shift in (2, 1, 3):
                share(p, f, shift, 0, 0, PIECE[f], torus.near(TURN[p][f], shift))
            return
        axis, half = TURN[p][f], FIRST[f]
        rest = PIECE[f] - half
        right, left = torus.near(axis, 1), torus.near(axis, -1)
        share(p, f, 0, 0, 0, half, right)
        share(p, f, 1, 0, half, rest, left)
        share(p, f, 2, 0, half, rest, right)
        share(p, f, 3, 0, 0, half, left)

    def relay_share(p, f):
        if f in DIRECT:
            return
        axis, half = TURN[p][f], FIRST[f]
        rest = PIECE[f] - half
        coming[p, f, 0].wait_recv()
        share(p, f, 4, -1, 0, half, torus.near(axis, 1))
        coming[p, f, 1].wait_recv()
        share(p, f, 5, 1, half, rest, torus.near(axis, -1))

    given = []

    def give(p, shift, offset, size, k):
        region = total.at[rows(block_row(p, 0, shift) + offset, size)]
        slot = p * 5 + k
        given.append(
            send(region, region, give_send.at[slot], give_recv.at[slot], torus.partner())
        )

    for p in range(PARTS):
        open_share(p, PHASES - 1)
    for f in DIRECT[::-1]:
        for p in range(PARTS):
            for shift in (1, 3, 2):
                coming[p, f, shift].wait_recv()
            open_share(p, f - 1)
    for p in range(PARTS):
        give(p, 0, 0, PIECE[0], 0)
    for p in range(PARTS):
        relay_share(p, 0)
    for p in range(PARTS):
        coming[p, 0, 2].wait_recv()
        give(p, -1, 0, PIECE[0], 1)
        coming[p, 0, 3].wait_recv()
        give(p, 1, 0, PIECE[0], 2)
    for p in range(PARTS):
        coming[p, 0, 4].wait_recv()
        give(p, 2, 0, FIRST[0], 3)
        coming[p, 0, 5].wait_recv()
        give(p, 2, FIRST[0], PIECE[0] - FIRST[0], 4)
    rim.wait()
    rim_out[...] = rim_buf[...]
    for copy in given:
        copy.wait_recv()
    for copy in sent:
        copy.wait_send()


def whole(n):
    return [pl.BlockSpec(memory_space=pltpu.VMEM)] * n


def combine(packed, rim_grad):
    dma = pltpu.SemaphoreType.DMA
    hops = PARTS * PHASES * HOPS
    scratch = [pltpu.VMEM((RIM, D), BF16), pltpu.VMEM((HALF, LANES), BF16)]
    scratch += [pltpu.VMEM((PARTS * 4 * n, LANES), F32) for n in PIECE]
    scratch += [pltpu.VMEM((PARTS * 4 * n, LANES), BF16) for n in PIECE]
    scratch += [pltpu.VMEM((12, n, LANES), BF16) for n in FIRST]
    scratch += [pltpu.VMEM((12, m - n, LANES), BF16) for m, n in zip(PIECE, FIRST)]
    scratch += [pltpu.VMEM((2, PARTS, 4, PIECE[1], LANES), BF16)]
    scratch += [dma((n,)) for n in (8, 8, 12, 12, hops, hops, hops, hops, 15, 15)]
    return pl.pallas_call(
        combine_kernel,
        out_shape=[
            jax.ShapeDtypeStruct((PACKED, LANES), BF16),
            jax.ShapeDtypeStruct((RIM, D), BF16),
        ],
        in_specs=whole(2),
        out_specs=whole(2),
        scratch_shapes=scratch,
        compiler_params=pltpu.CompilerParams(
            collective_id=1, has_side_effects=True, vmem_limit_bytes=24 * 1024 * 1024
        ),
        name="combine",
    )(packed, rim_grad)


def finish_kernel(
    total,
    rim_in,
    base,
    node_grad,
    g_edge_in,
    g_edge_out,
    g_node_in,
    g_node_out,
    gain_edge,
    gain_node,
    sems,
):
    copies = []
    for out, at in (
        (g_edge_in, AT_EDGE_IN),
        (g_edge_out, AT_EDGE_OUT),
        (g_node_in, AT_NODE_IN),
        (g_node_out, AT_NODE_OUT),
    ):
        size = out.shape[0]
        for j in range(4):
            copies.append(
                pltpu.make_async_copy(
                    total.at[pl.ds(at + j * size, size)],
                    out.at[:, pl.ds(j * LANES, LANES)],
                    sems.at[len(copies)],
                )
            )
            copies[-1].start()
    tail = total[pl.ds(AT_GAINS, 16)].astype(F32)
    for j in range(4):
        gain_edge[:, pl.ds(j * LANES, LANES)] = tail[j : j + 1]
        gain_node[:, pl.ds(j * LANES, LANES)] = tail[4 + j : 5 + j]
    node_grad[...] = (base[...] + dot(rim_picks(1), rim_in[...])).astype(BF16)
    for copy in copies:
        copy.wait()


def finish(total, rim_in, base):
    shapes = [
        ((OWN, D), BF16),
        ((3 * D, D), BF16),
        ((D, D), BF16),
        ((2 * D, D), BF16),
        ((D, D), BF16),
        ((1, D), F32),
        ((1, D), F32),
    ]
    anywhere = [pl.BlockSpec(memory_space=pl.ANY)] * 4
    return pl.pallas_call(
        finish_kernel,
        out_shape=[jax.ShapeDtypeStruct(s, t) for s, t in shapes],
        in_specs=whole(3),
        out_specs=whole(1) + anywhere + whole(2),
        scratch_shapes=[pltpu.SemaphoreType.DMA((16,))],
        compiler_params=pltpu.CompilerParams(vmem_limit_bytes=16 * 1024 * 1024),
        name="finish",
    )(total, rim_in, base)


RIM_SCRATCH = [
    pltpu.VMEM((RIM, D), BF16),
    pltpu.VMEM((RIM, D), BF16),
    pltpu.SemaphoreType.DMA((len(ROUTES),)),
    pltpu.SemaphoreType.DMA((len(ROUTES),)),
]


def halo(nodes):
    return pl.pallas_call(
        halo_kernel,
        out_shape=jax.ShapeDtypeStruct((RIM, D), BF16),
        in_specs=whole(1),
        out_specs=whole(1)[0],
        scratch_shapes=RIM_SCRATCH,
        compiler_params=pltpu.CompilerParams(
            collective_id=0, has_side_effects=True, vmem_limit_bytes=8 * 1024 * 1024
        ),
        cost_estimate=pl.CostEstimate(flops=6 * 10**9, bytes_accessed=2**20, transcendentals=0),
        name="halo",
    )(nodes)


def normalize(values):
    average = jnp.mean(values, -1, keepdims=True)
    centred = values - average
    spread = jnp.mean(centred * centred, -1, keepdims=True)
    inverse = lax.rsqrt(spread + EPS)
    return centred * inverse, inverse


def norm_backward(scaled, standard, inverse):
    return inverse * (
        scaled
        - jnp.mean(scaled, -1, keepdims=True)
        - standard * jnp.mean(scaled * standard, -1, keepdims=True)
    )


def silu_parts(values):
    logistic = 1.0 / (1.0 + jnp.exp(-values))
    hidden = values * logistic
    return hidden, logistic * (1.0 + values * (1.0 - logistic))


def cell_rows(senders):
    row = (senders * 1928) >> 16
    col = senders - row * 34
    left, right = col == 0, col == 33
    top, bottom = row == 0, row == 17
    place = (row - 1) * 32 + col - 1
    place = jnp.where(top, OWN + col - 1, place)
    place = jnp.where(bottom, OWN + 32 + col - 1, place)
    place = jnp.where(left, OWN + 64 + row - 1, place)
    place = jnp.where(right, OWN + 80 + row - 1, place)
    place = jnp.where(jnp.logical_and(top, left), OWN + 96, place)
    place = jnp.where(jnp.logical_and(top, right), OWN + 112, place)
    place = jnp.where(jnp.logical_and(bottom, left), OWN + 128, place)
    return jnp.where(jnp.logical_and(bottom, right), OWN + 144, place)


def one_hot(mask):
    return jnp.where(mask, 1.0, 0.0).astype(BF16)


def picks_by_slot(ids, width):
    parts = []
    for k in range(PER):
        column = jnp.broadcast_to(ids[k : k + 1], (SLOTS, SLOTS)).T
        lanes = lax.broadcasted_iota(jnp.int32, (SLOTS, SLOTS), 1)
        parts.append(
            jnp.concatenate([one_hot(column == lanes + s) for s in range(0, width, SLOTS)], axis=1)
        )
    return jnp.concatenate(parts, axis=0)


def picks_by_row(ids, height):
    rows = lax.broadcasted_iota(jnp.int32, (height, SLOTS), 0)
    return jnp.concatenate([one_hot(rows == ids[k : k + 1]) for k in range(PER)], axis=1)


def local_kernel(
    counts,
    nodes,
    rim,
    edges,
    senders,
    receivers,
    cotangent,
    w_edge_in,
    w_edge_out,
    w_node_in,
    w_node_out,
    gain_edge,
    gain_node,
    node_out_far,
    edge_out_far,
    edge_grad_far,
    base,
    rim_grad,
    packed,
    node_out,
    edge_out,
    edge_grad,
    sems,
    proj,
    cells,
    hidden_all,
    slope_all,
    std_all,
    inv_all,
    agg,
    acc_send,
    acc_recv,
    acc_in,
    acc_out,
    grad_agg,
):
    def chunk_out(step, near, far, at):
        span = rows(step * CHUNK, CHUNK)
        return pltpu.make_async_copy(near.at[span], far.at[span], sems.at[at + step])

    node_copy = pltpu.make_async_copy(node_out, node_out_far, sems.at[2 * STEPS])

    def pack(at, size, row, value):
        value = value.astype(BF16)
        for j in range(4):
            onto = pl.ds(at + j * size + row, value.shape[0])
            packed[onto] = value[:, j * LANES : (j + 1) * LANES]

    own = nodes[...]
    cells[...] = cell_rows(senders[...])
    w_mid = w_edge_in[pl.ds(D, D)]
    proj[pl.ds(0, OWN)] = dot(own, w_mid).astype(BF16)
    proj[pl.ds(OWN, RIM)] = dot(rim[...], w_mid).astype(BF16)
    proj[pl.ds(CELLS, RIM_PAD - RIM)] = jnp.zeros((RIM_PAD - RIM, D), BF16)
    proj[pl.ds(OWN + RIM_PAD, OWN)] = dot(own, w_edge_in[pl.ds(2 * D, D)]).astype(BF16)

    agg[...] = jnp.zeros_like(agg)
    acc_send[...] = jnp.zeros_like(acc_send)
    acc_recv[...] = jnp.zeros_like(acc_recv)
    acc_in[...] = jnp.zeros_like(acc_in)
    acc_out[...] = jnp.zeros_like(acc_out)

    def live(step):
        slot = lax.broadcasted_iota(jnp.int32, (SLOTS, 1), 0)
        return jnp.concatenate(
            [jnp.where(slot < counts[step * PER + k], 1.0, 0.0) for k in range(PER)], axis=0
        )

    def forward(step, carry):
        span = pl.ds(pl.multiple_of(step * CHUNK, CHUNK), CHUNK)
        blocks = pl.ds(step * PER, PER)
        block = edges[span]
        recv_ids = receivers[blocks]
        picks = jnp.concatenate(
            [picks_by_slot(cells[blocks], OWN + RIM_PAD), picks_by_slot(recv_ids, OWN)], axis=1
        )
        pre = dot(block, w_edge_in[pl.ds(0, D)]) + dot(picks, proj[...])
        hidden, slope = silu_parts(pre)
        hidden = hidden.astype(BF16)
        hidden_all[span] = hidden
        slope_all[span] = slope
        standard, inverse = normalize(dot(hidden, w_edge_out[...]))
        std_all[span] = standard
        inv_all[span] = inverse
        message = standard * gain_edge[...] * live(step)
        edge_out[span] = (block.astype(F32) + message).astype(BF16)
        chunk_out(step, edge_out, edge_out_far, 0).start()
        agg[...] += dot(picks_by_row(recv_ids, OWN), message.astype(BF16))
        return carry

    lax.fori_loop(0, STEPS, forward, 0, unroll=True)

    sums = agg[...].astype(BF16)
    node_pre = dot(own, w_node_in[pl.ds(0, D)]) + dot(sums, w_node_in[pl.ds(D, D)])
    node_hidden, node_slope = silu_parts(node_pre)
    node_hidden = node_hidden.astype(BF16)
    node_std, node_inv = normalize(dot(node_hidden, w_node_out[...]))
    node_out[...] = (own.astype(F32) + node_std * gain_node[...]).astype(BF16)
    node_copy.start()
    upstream = cotangent[...]
    gain_sum_node = jnp.sum(upstream * node_std, 0, keepdims=True)
    grad_mlp = norm_backward(upstream * gain_node[...], node_std, node_inv).astype(BF16)
    pack(AT_NODE_OUT, D, 0, dot_at(node_hidden, grad_mlp))
    grad_node_pre = (dot_bt(grad_mlp, w_node_out[...]) * node_slope).astype(BF16)
    pack(AT_NODE_IN, 2 * D, 0, dot_at(own, grad_node_pre))
    pack(AT_NODE_IN, 2 * D, D, dot_at(sums, grad_node_pre))
    base[...] = upstream + dot_bt(grad_node_pre, w_node_in[pl.ds(0, D)])
    grad_agg[...] = dot_bt(grad_node_pre, w_node_in[pl.ds(D, D)]).astype(BF16)

    def backward(step, gain_sum):
        span = pl.ds(pl.multiple_of(step * CHUNK, CHUNK), CHUNK)
        blocks = pl.ds(step * PER, PER)
        recv_ids = receivers[blocks]
        standard = std_all[span]
        incoming = dot(picks_by_slot(recv_ids, OWN), grad_agg[...]) * live(step)
        gain_sum = gain_sum + jnp.sum(incoming * standard, 0, keepdims=True)
        grad_norm = norm_backward(incoming * gain_edge[...], standard, inv_all[span]).astype(BF16)
        acc_out[...] += dot_at(hidden_all[span], grad_norm)
        grad_pre = (dot_bt(grad_norm, w_edge_out[...]) * slope_all[span]).astype(BF16)
        acc_in[...] += dot_at(edges[span], grad_pre)
        edge_grad[span] = dot_bt(grad_pre, w_edge_in[pl.ds(0, D)]).astype(BF16)
        chunk_out(step, edge_grad, edge_grad_far, STEPS).start()
        acc_send[...] += dot(picks_by_row(cells[blocks], CELLS), grad_pre)
        acc_recv[...] += dot(picks_by_row(recv_ids, OWN), grad_pre)
        return gain_sum

    gain_sum_edge = lax.fori_loop(0, STEPS, backward, jnp.zeros((1, D), F32), unroll=True)
    tail = [v[:, j * LANES : (j + 1) * LANES] for v in (gain_sum_edge, gain_sum_node) for j in range(4)]
    tail = jnp.concatenate(tail + [jnp.zeros((PACKED - AT_GAINS - 8, LANES), F32)], axis=0)
    packed[pl.ds(AT_GAINS, PACKED - AT_GAINS)] = tail.astype(BF16)
    pack(AT_EDGE_OUT, D, 0, acc_out[...])
    pack(AT_EDGE_IN, 3 * D, 0, acc_in[...])
    by_send = acc_send[...].astype(BF16)
    by_recv = acc_recv[...].astype(BF16)
    pack(AT_EDGE_IN, 3 * D, D, dot_at(own, by_send[:OWN]) + dot_at(rim[...], by_send[OWN:]))
    pack(AT_EDGE_IN, 3 * D, 2 * D, dot_at(own, by_recv))
    rim_grad[...] = dot_bt(by_send[OWN:], w_mid).astype(BF16)
    base[...] += dot_bt(by_send[:OWN], w_mid) + dot_bt(by_recv, w_edge_in[pl.ds(2 * D, D)])
    node_copy.wait()
    for step in range(STEPS):
        chunk_out(step, edge_out, edge_out_far, 0).wait()
        chunk_out(step, edge_grad, edge_grad_far, STEPS).wait()


def local(counts, *rest):
    shapes = [
        ((OWN, D), BF16),
        ((EDGES, D), BF16),
        ((EDGES, D), BF16),
        ((OWN, D), F32),
        ((RIM, D), BF16),
        ((PACKED, LANES), BF16),
    ]
    scratch = [
        ((TABLE, D), BF16),
        ((BLOCKS, SLOTS), jnp.int32),
        ((EDGES, D), BF16),
        ((EDGES, D), F32),
        ((EDGES, D), F32),
        ((EDGES, 1), F32),
        ((OWN, D), F32),
        ((CELLS, D), F32),
        ((OWN, D), F32),
        ((D, D), F32),
        ((D, D), F32),
        ((OWN, D), BF16),
    ]
    return pl.pallas_call(
        local_kernel,
        out_shape=[jax.ShapeDtypeStruct(s, t) for s, t in shapes],
        in_specs=[pl.BlockSpec(memory_space=pltpu.SMEM)] + whole(len(rest)),
        out_specs=[pl.BlockSpec(memory_space=pl.ANY)] * 3 + whole(3),
        scratch_shapes=[pltpu.VMEM(s, t) for s, t in shapes[:3]]
        + [pltpu.SemaphoreType.DMA((2 * STEPS + 1,))]
        + [pltpu.VMEM(s, t) for s, t in scratch],
        compiler_params=pltpu.CompilerParams(vmem_limit_bytes=VMEM_LIMIT),
        name="local",
    )(counts, *rest)


def shards(
    nodes,
    edges,
    senders,
    receivers,
    counts,
    cotangent,
    w_edge_in,
    w_edge_out,
    w_node_in,
    w_node_out,
    gain_edge,
    gain_node,
):
    own = nodes.reshape(OWN, D)
    rim = halo(own)
    node_out, edge_out, edge_grad, base, rim_grad, packed = local(
        counts.reshape(BLOCKS),
        own,
        rim,
        edges.reshape(EDGES, D),
        senders.reshape(BLOCKS, SLOTS),
        receivers.reshape(BLOCKS, SLOTS),
        cotangent.reshape(OWN, D),
        w_edge_in,
        w_edge_out,
        w_node_in,
        w_node_out,
        gain_edge.reshape(1, D),
        gain_node.reshape(1, D),
    )
    total, rim_in = combine(packed, rim_grad)
    node_grad, *summed, gain_sum_edge, gain_sum_node = finish(total, rim_in, base)
    return (
        node_out.reshape(nodes.shape),
        edge_out.reshape(edges.shape),
        node_grad.reshape(nodes.shape),
        edge_grad.reshape(edges.shape),
        *summed,
        gain_sum_edge.reshape(D),
        gain_sum_node.reshape(D),
    )


def solution(mesh):
    in_specs = (
        P("lat", "lon", None),
        P("lat", "lon", None, None, None),
        P("lat", "lon", None, None),
        P("lat", "lon", None, None),
        P("lat", "lon", None),
        P("lat", "lon", None),
        P(),
        P(),
        P(),
        P(),
        P(),
        P(),
    )
    out_specs = (
        P("lat", "lon", None),
        P("lat", "lon", None, None, None),
        P("lat", "lon", None),
        P("lat", "lon", None, None, None),
        P(),
        P(),
        P(),
        P(),
        P(),
        P(),
    )
    return jax.shard_map(shards, mesh=mesh, in_specs=in_specs, out_specs=out_specs, check_vma=False)
```
